32 devices in a mesh: pair: 2 (over x), tp: 4 (over z), side: 4 (over y, core).
Axes of the slice: x: 2, y: 2, z: 4, core: 2. Of those that a mesh axis runs over, the one named last changes fastest.
Arguments:
- prompt_x: bfloat16 [8192, 2048], P(('pair', 'side')), parts along dimension 0
- s_len: int32 [8], P(('pair', 'side')), parts along dimension 0
- w_qkv_pre: bfloat16 [2, 2048, 3, 16, 128], P(None, None, None, 'tp')
- w_out_pre: bfloat16 [2, 16, 128, 2048], P(None, 'tp')
- w_gu_pre: bfloat16 [2, 2, 5504, 2048], P(None, None, 'tp')
- w_down_pre: bfloat16 [2, 5504, 2048], P(None, 'tp')
- gain_pre: float32 [2, 2, 2048], replicated
- dec_tokens: bfloat16 [64, 2048], P(('pair', 'side')), parts along dimension 0
- k_cache: bfloat16 [2, 64, 256, 4, 4, 128], P(None, ('pair', 'side'), None, None, 'tp'), parts along dimension 1
- v_cache: bfloat16 [2, 64, 256, 4, 4, 128], P(None, ('pair', 'side'), None, None, 'tp'), parts along dimension 1
- c_len: int32 [64], P(('pair', 'side')), parts along dimension 0
- w_qkv_dec: bfloat16 [2, 2048, 3, 4, 4, 128], P(None, None, None, None, 'tp')
- w_out_dec: bfloat16 [2, 4, 4, 128, 2048], P(None, None, 'tp')
- w_gu_dec: bfloat16 [2, 2, 5504, 2048], P(None, None, 'tp')
- w_down_dec: bfloat16 [2, 5504, 2048], P(None, 'tp')
- gain_dec: float32 [2, 2, 2048], replicated
Outputs:
- output 1: bfloat16 [8192, 2048], P(('pair', 'side')), parts along dimension 0
- output 2: bfloat16 [64, 2048], P(('pair', 'side')), parts along dimension 0
- output 3: bfloat16 [2, 8192, 4, 4, 128], P(None, ('pair', 'side'), None, 'tp'), parts along dimension 1
- output 4: bfloat16 [2, 8192, 4, 4, 128], P(None, ('pair', 'side'), None, 'tp'), parts along dimension 1
- output 5: bfloat16 [2, 64, 256, 4, 4, 128], P(None, ('pair', 'side'), None, None, 'tp'), parts along dimension 1
- output 6: bfloat16 [2, 64, 256, 4, 4, 128], P(None, ('pair', 'side'), None, None, 'tp'), parts along dimension 1
There are 2 independent parts. The reference program is written for one: setup_inputs(seed, part) draws one part's arguments, and reference() takes and returns one part's arrays. A program takes and returns all parts, laid end to end along the dimension named above; an argument that names none is the same for every part.
All inputs are finite; a program needn't handle non-finite values.
Results may differ from the reference program's by a relative error of at most 0.02.
Values are sent between devices in bfloat16 or wider.
A program may use at most 1 GiB of HBM per device.

```python
import jax
import jax.numpy as jnp
from jax import lax

D = 2048
HEADS = 16
HEAD = 128
FF = 5504
LAYERS = 2
PROMPT = 1024
BATCH = 8
CACHE = 256
TP_SIZE = 4
SIDES = 4

EPSILON = 1e-6
THETA = 10000.0
QK_GAIN = 1.5
OUT_GAIN = 2.0
MASKED = -1e30


def draw_int_inputs(len_key, cache_key):
    low_prompt = PROMPT // 2
    len_keys = jax.random.split(len_key, 2)
    s_len = jax.random.randint(len_keys[0], (SIDES,), low_prompt, PROMPT + 1, dtype=jnp.int32)
    slot_top = jax.random.randint(len_keys[1], (), 0, SIDES, dtype=jnp.int32)
    s_len = s_len.at[slot_top].set(PROMPT).at[(slot_top + 1) % SIDES].set(low_prompt)
    low_cache = CACHE // 4
    row_total = SIDES * BATCH
    cache_keys = jax.random.split(cache_key, 2)
    c_len = jax.random.randint(cache_keys[0], (row_total,), low_cache, CACHE, dtype=jnp.int32)
    row_top = jax.random.randint(cache_keys[1], (), 0, row_total, dtype=jnp.int32)
    c_len = c_len.at[row_top].set(CACHE - 1).at[(row_top + 1) % row_total].set(low_cache)
    return s_len, c_len


def draw_weights(weight_key):
    weight_keys = jax.random.split(weight_key, 5)
    qkv_scale = jnp.array([QK_GAIN, QK_GAIN, 1.0], jnp.float32)[:, None, None] * D ** -0.5
    w_qkv = (jax.random.normal(weight_keys[0], (LAYERS, D, 3, HEADS, HEAD), jnp.float32) * qkv_scale).astype(jnp.bfloat16)
    w_out = (jax.random.normal(weight_keys[1], (LAYERS, HEADS, HEAD, D), jnp.float32) * (OUT_GAIN * (HEADS * HEAD) ** -0.5)).astype(jnp.bfloat16)
    w_gu = (jax.random.normal(weight_keys[2], (LAYERS, 2, FF, D), jnp.float32) * D ** -0.5).astype(jnp.bfloat16)
    w_down = (jax.random.normal(weight_keys[3], (LAYERS, FF, D), jnp.float32) * FF ** -0.5).astype(jnp.bfloat16)
    gains = jax.random.uniform(weight_keys[4], (LAYERS, 2, D), jnp.float32, 0.5, 1.5)
    return w_qkv, w_out, w_gu, w_down, gains


def setup_inputs(seed: int = 0, part: int = 0) -> dict:
    shared_keys = jax.random.split(jax.random.key(seed + 1), 2)
    part_keys = jax.random.split(jax.random.fold_in(jax.random.key(seed), part), 6)
    heads_tp = HEADS // TP_SIZE
    w_qkv_pre, w_out_pre, w_gu_pre, w_down_pre, gain_pre = draw_weights(shared_keys[0])
    w_qkv_dec, w_out_dec, w_gu_dec, w_down_dec, gain_dec = draw_weights(shared_keys[1])
    s_len, c_len = draw_int_inputs(part_keys[0], part_keys[1])
    prompt_x = jax.random.normal(part_keys[2], (SIDES * PROMPT, D), jnp.float32).astype(jnp.bfloat16)
    dec_tokens = jax.random.normal(part_keys[3], (SIDES * BATCH, D), jnp.float32).astype(jnp.bfloat16)
    cache_shape = (LAYERS, SIDES * BATCH, CACHE, heads_tp, TP_SIZE, HEAD)
    k_cache = (jax.random.normal(part_keys[4], cache_shape, jnp.float32) * QK_GAIN).astype(jnp.bfloat16)
    v_cache = jax.random.normal(part_keys[5], cache_shape, jnp.float32).astype(jnp.bfloat16)
    return {'prompt_x': prompt_x, 's_len': s_len, 'w_qkv_pre': w_qkv_pre, 'w_out_pre': w_out_pre, 'w_gu_pre': w_gu_pre, 'w_down_pre': w_down_pre, 'gain_pre': gain_pre, 'dec_tokens': dec_tokens, 'k_cache': k_cache, 'v_cache': v_cache, 'c_len': c_len, 'w_qkv_dec': w_qkv_dec.reshape(LAYERS, D, 3, heads_tp, TP_SIZE, HEAD), 'w_out_dec': w_out_dec.reshape(LAYERS, heads_tp, TP_SIZE, HEAD, D), 'w_gu_dec': w_gu_dec, 'w_down_dec': w_down_dec, 'gain_dec': gain_dec}


def rms_norm(hidden, gain_vec):
    hid_f32 = hidden.astype(jnp.float32)
    inv_rms = lax.rsqrt(jnp.mean(hid_f32 * hid_f32, axis=-1, keepdims=True) + EPSILON)
    return (hid_f32 * inv_rms * gain_vec).astype(jnp.bfloat16)


def add_residual(hidden, update):
    return (hidden.astype(jnp.float32) + update.astype(jnp.float32)).astype(jnp.bfloat16)


def rope_tables(positions):
    half_dim = HEAD // 2
    inv_freq = THETA ** (-jnp.arange(half_dim, dtype=jnp.float32) * 2.0 / HEAD)
    angles = positions.astype(jnp.float32)[:, None] * inv_freq[None, :]
    return jnp.cos(angles), jnp.sin(angles)


def apply_rope(values_in, cos_tab, sin_tab):
    half_dim = values_in.shape[-1] // 2
    lower_half = values_in[..., :half_dim]
    upper_half = values_in[..., half_dim:]
    cos_b = cos_tab[:, None, :]
    sin_b = sin_tab[:, None, :]
    return jnp.concatenate([lower_half * cos_b - upper_half * sin_b, upper_half * cos_b + lower_half * sin_b], axis=-1)


def mlp_block(hidden, gain_vec, w_gu, w_down):
    normed = rms_norm(hidden, gain_vec)
    gate_up = jnp.einsum('sd,kfd->skf', normed.astype(jnp.float32), w_gu.astype(jnp.float32))
    gate_val = gate_up[:, 0].astype(jnp.bfloat16).astype(jnp.float32)
    up_val = gate_up[:, 1].astype(jnp.bfloat16).astype(jnp.float32)
    activated = (jax.nn.silu(gate_val) * up_val).astype(jnp.bfloat16)
    down_out = jnp.dot(activated, w_down, preferred_element_type=jnp.float32).astype(jnp.bfloat16)
    return add_residual(hidden, down_out)


def prefill_one(x_inst, s_valid, w_qkv, w_out, w_gu, w_down, gains):
    positions = jnp.arange(PROMPT)
    cos_tab, sin_tab = rope_tables(positions)
    allowed = (positions[None, :] <= positions[:, None]) & (positions[None, :] < s_valid)

    def head_attention(head_in):
        q_head, k_head, v_head = head_in
        scores = jnp.einsum('qe,ke->qk', q_head.astype(jnp.float32), k_head.astype(jnp.float32)) * HEAD ** -0.5
        scores = jnp.where(allowed, scores, MASKED)
        prob_bf = jax.nn.softmax(scores, axis=-1).astype(jnp.bfloat16)
        return jnp.einsum('qk,ke->qe', prob_bf.astype(jnp.float32), v_head.astype(jnp.float32)).astype(jnp.bfloat16)

    def layer_step(hidden, layer_in):
        wqkv_l, wout_l, wgu_l, wdown_l, gain_l = layer_in
        normed = rms_norm(hidden, gain_l[0])
        qkv_out = jnp.einsum('sd,dkhe->skhe', normed.astype(jnp.float32), wqkv_l.astype(jnp.float32))
        queries = apply_rope(qkv_out[:, 0], cos_tab, sin_tab).astype(jnp.bfloat16)
        keys_new = apply_rope(qkv_out[:, 1], cos_tab, sin_tab).astype(jnp.bfloat16)
        values_new = qkv_out[:, 2].astype(jnp.bfloat16)
        context = lax.map(head_attention, (queries.transpose(1, 0, 2), keys_new.transpose(1, 0, 2), values_new.transpose(1, 0, 2)))
        attn_out = jnp.einsum('hse,hed->sd', context.astype(jnp.float32), wout_l.astype(jnp.float32)).astype(jnp.bfloat16)
        hidden = add_residual(hidden, attn_out)
        hidden = mlp_block(hidden, gain_l[1], wgu_l, wdown_l)
        return hidden, (keys_new, values_new)

    return lax.scan(layer_step, x_inst, (w_qkv, w_out, w_gu, w_down, gains))


def decode_rows(tokens, k_cache, v_cache, c_len, w_qkv, w_out, w_gu, w_down, gains):
    row_total = tokens.shape[0]
    cos_tab, sin_tab = rope_tables(c_len)
    cache_pos = jnp.arange(CACHE)
    k_flat = k_cache.reshape(LAYERS, row_total, CACHE, HEADS, HEAD)
    v_flat = v_cache.reshape(LAYERS, row_total, CACHE, HEADS, HEAD)
    wqkv_flat = w_qkv.reshape(LAYERS, D, 3, HEADS, HEAD)
    wout_flat = w_out.reshape(LAYERS, HEADS, HEAD, D)
    write_at = (cache_pos[None, :] == c_len[:, None])[:, :, None, None]

    def row_attention(row_in):
        q_row, k_row, v_row, kc_row, vc_row, len_row = row_in
        cache_scores = jnp.einsum('he,the->ht', q_row.astype(jnp.float32), kc_row.astype(jnp.float32)) * HEAD ** -0.5
        cache_scores = jnp.where(cache_pos[None, :] < len_row, cache_scores, MASKED)
        self_score = jnp.sum(q_row.astype(jnp.float32) * k_row.astype(jnp.float32), axis=-1) * HEAD ** -0.5
        joint_scores = jnp.concatenate([cache_scores, self_score[:, None]], axis=1)
        prob_bf = jax.nn.softmax(joint_scores, axis=-1).astype(jnp.bfloat16).astype(jnp.float32)
        context = jnp.einsum('ht,the->he', prob_bf[:, :CACHE], vc_row.astype(jnp.float32)) + prob_bf[:, CACHE:] * v_row.astype(jnp.float32)
        return context.astype(jnp.bfloat16)

    def layer_step(hidden, layer_in):
        wqkv_l, wout_l, wgu_l, wdown_l, gain_l, kc_l, vc_l = layer_in
        normed = rms_norm(hidden, gain_l[0])
        qkv_out = jnp.einsum('bd,dkhe->bkhe', normed.astype(jnp.float32), wqkv_l.astype(jnp.float32))
        queries = apply_rope(qkv_out[:, 0], cos_tab, sin_tab).astype(jnp.bfloat16)
        k_tok = apply_rope(qkv_out[:, 1], cos_tab, sin_tab).astype(jnp.bfloat16)
        v_tok = qkv_out[:, 2].astype(jnp.bfloat16)
        context = lax.map(row_attention, (queries, k_tok, v_tok, kc_l, vc_l, c_len))
        attn_out = jnp.einsum('bhe,hed->bd', context.astype(jnp.float32), wout_l.astype(jnp.float32)).astype(jnp.bfloat16)
        hidden = add_residual(hidden, attn_out)
        hidden = mlp_block(hidden, gain_l[1], wgu_l, wdown_l)
        kc_next = jnp.where(write_at, k_tok[:, None], kc_l)
        vc_next = jnp.where(write_at, v_tok[:, None], vc_l)
        return hidden, (kc_next, vc_next)

    final_tokens, (kc_all, vc_all) = lax.scan(layer_step, tokens, (wqkv_flat, wout_flat, w_gu, w_down, gains, k_flat, v_flat))
    return final_tokens, kc_all.reshape(k_cache.shape), vc_all.reshape(v_cache.shape)


def reference(prompt_x, s_len, w_qkv_pre, w_out_pre, w_gu_pre, w_down_pre, gain_pre, dec_tokens, k_cache, v_cache, c_len, w_qkv_dec, w_out_dec, w_gu_dec, w_down_dec, gain_dec):
    prompts = prompt_x.reshape(SIDES, PROMPT, D)

    def run_instance(inst_in):
        x_inst, s_valid = inst_in
        final_hidden, (k_all, v_all) = prefill_one(x_inst, s_valid, w_qkv_pre, w_out_pre, w_gu_pre, w_down_pre, gain_pre)
        return final_hidden, k_all, v_all

    final_hidden, k_all, v_all = lax.map(run_instance, (prompts, s_len))
    half_sides = SIDES // 2
    prompt_shape = (LAYERS, SIDES * PROMPT, HEADS // TP_SIZE, TP_SIZE, HEAD)
    k_prompt = jnp.roll(k_all, half_sides, axis=0).transpose(1, 0, 2, 3, 4).reshape(prompt_shape)
    v_prompt = jnp.roll(v_all, half_sides, axis=0).transpose(1, 0, 2, 3, 4).reshape(prompt_shape)
    dec_out, k_cache_new, v_cache_new = decode_rows(dec_tokens, k_cache, v_cache, c_len, w_qkv_dec, w_out_dec, w_gu_dec, w_down_dec, gain_dec)
    return (final_hidden.reshape(SIDES * PROMPT, D), dec_out, k_prompt, v_prompt, k_cache_new, v_cache_new)
```

```python
import jax
import jax.numpy as jnp
from jax import lax
from jax.experimental import pallas as pl
from jax.experimental.pallas import tpu as pltpu
from jax.sharding import PartitionSpec as P

EPSILON = 1e-6
THETA = 10000.0
MASKED = -1e30
CTX_ROWS = 128
SUM_ROWS = 32
DOT_ROWS = 128
DOT_COLS = 512
VMEM_BYTES = 56 * 1024 * 1024
MESH = pl.DeviceIdType.MESH


def greet(me, tp_size):
    barrier = pltpu.get_barrier_semaphore()
    for off in range(1, tp_size):
        pl.semaphore_signal(barrier, inc=1, device_id={'tp': lax.rem(me + off, tp_size)}, device_id_type=MESH)
    pl.semaphore_wait(barrier, tp_size - 1)


def to_peer(src, dst, send_sem, recv_sem, peer):
    return pltpu.make_async_remote_copy(src_ref=src, dst_ref=dst, send_sem=send_sem, recv_sem=recv_sem, device_id={'tp': peer}, device_id_type=MESH)


def share_small(me, tp_size, part_ref, held, send_sems, recv_sems):
    for off in range(1, tp_size):
        peer = lax.rem(me + off, tp_size)
        to_peer(part_ref, held.at[me], send_sems.at[off - 1], recv_sems.at[me], peer).start()


def sum_small(me, tp_size, part_ref, held, send_sems, recv_sems, out_ref):
    for off in range(1, tp_size):
        peer = lax.rem(me + off, tp_size)
        copy = to_peer(part_ref, held.at[peer], send_sems.at[off - 1], recv_sems.at[peer], peer)
        copy.wait_send()
        copy.wait_recv()
    held[me] = part_ref[...]
    total = held[0]
    for idx in range(1, tp_size):
        total = total + held[idx]
    out_ref[...] = total.astype(out_ref.dtype)


def ctx_kernel(tp_size, ctx_ref, part_ref, full_ref, small_ref, held, up_send, up_recv, dn_send, dn_recv, sm_send, sm_recv):
    me = lax.axis_index('tp')
    last = tp_size - 1
    chunks = ctx_ref.shape[0] // CTX_ROWS
    greet(me, tp_size)
    share_small(me, tp_size, part_ref, held, sm_send, sm_recv)

    def rows_of(chunk):
        return pl.ds(pl.multiple_of(chunk * CTX_ROWS, CTX_ROWS), CTX_ROWS)

    def tick(step, carry):
        for back in range(tp_size):
            chunk = step - back
            inside = (chunk >= 0) & (chunk < chunks)
            for sign, send, recv in ((1, up_send, up_recv), (-1, dn_send, dn_recv)):
                shard = me - sign * back
                peer = me + sign
                has = inside & (shard >= 0) & (shard <= last)
                more = has & (peer >= 0) & (peer <= last)
                rows = rows_of(chunk)
                if back == 0:
                    @pl.when(more)
                    def _():
                        to_peer(ctx_ref.at[rows], full_ref.at[me, rows], send.at[0, chunk], recv.at[0, chunk], peer).start()
                else:
                    @pl.when(has)
                    def _():
                        to_peer(ctx_ref.at[rows], full_ref.at[shard, rows], send.at[back - 1, chunk], recv.at[back - 1, chunk], me).wait_recv()
                    if back < last:
                        @pl.when(more)
                        def _():
                            to_peer(full_ref.at[shard, rows], full_ref.at[shard, rows], send.at[back, chunk], recv.at[back, chunk], peer).start()
        return carry

    lax.fori_loop(0, chunks + last, tick, 0)
    full_ref[me] = ctx_ref[...]

    def drain(chunk, carry):
        for back in range(last):
            for sign, send, recv in ((1, up_send, up_recv), (-1, dn_send, dn_recv)):
                shard = me - sign * back
                peer = me + sign

                @pl.when((shard >= 0) & (shard <= last) & (peer >= 0) & (peer <= last))
                def _():
                    to_peer(ctx_ref.at[rows_of(chunk)], full_ref.at[me, rows_of(chunk)], send.at[back, chunk], recv.at[back, chunk], peer).wait_send()
        return carry

    lax.fori_loop(0, chunks, drain, 0)
    sum_small(me, tp_size, part_ref, held, sm_send, sm_recv, small_ref)


def gather_ctx(ctx, small_part, tp_size):
    rows, width = ctx.shape
    chunks = rows // CTX_ROWS
    last = tp_size - 1
    vmem = pl.BlockSpec(memory_space=pltpu.VMEM)
    return pl.pallas_call(
        lambda *refs: ctx_kernel(tp_size, *refs),
        out_shape=(jax.ShapeDtypeStruct((tp_size, rows, width), ctx.dtype), jax.ShapeDtypeStruct(small_part.shape, jnp.bfloat16)),
        in_specs=[vmem, vmem],
        out_specs=(vmem, vmem),
        scratch_shapes=[pltpu.VMEM((tp_size,) + small_part.shape, jnp.float32)] + [pltpu.SemaphoreType.DMA((last, chunks))] * 4 + [pltpu.SemaphoreType.DMA((last,)), pltpu.SemaphoreType.DMA((tp_size,))],
        compiler_params=pltpu.CompilerParams(collective_id=0, has_side_effects=True, vmem_limit_bytes=VMEM_BYTES),
        cost_estimate=pl.CostEstimate(flops=70_000_000_000, bytes_accessed=rows * width * 10, transcendentals=0),
        name='ctx_gather',
    )(ctx, small_part)


def sum_kernel(tp_size, act_ref, wd_ref, hid_ref, part_ref, out_ref, small_ref, total, came, held, up_send, up_recv, dn_send, dn_recv, gu_send, gu_recv, gd_send, gd_recv, sm_send, sm_recv):
    me = lax.axis_index('tp')
    last = tp_size - 1
    half = hid_ref.shape[0] // 2
    chunks = half // SUM_ROWS
    per_dot = DOT_ROWS // SUM_ROWS
    width = hid_ref.shape[1]
    greet(me, tp_size)
    share_small(me, tp_size, part_ref, held, sm_send, sm_recv)
    streams = ((1, half, up_send, up_recv, gu_send, gu_recv), (-1, 0, dn_send, dn_recv, gd_send, gd_recv))

    def tick(step, carry):
        @pl.when((lax.rem(step, per_dot) == 0) & (step < chunks))
        def _():
            for base in (half, 0):
                rows = pl.ds(pl.multiple_of(base + step * SUM_ROWS, SUM_ROWS), DOT_ROWS)

                def columns(idx, inner):
                    cols = pl.ds(pl.multiple_of(idx * DOT_COLS, DOT_COLS), DOT_COLS)
                    total[rows, cols] = jnp.dot(act_ref[rows, :], wd_ref[:, cols], preferred_element_type=jnp.float32)
                    return inner

                lax.fori_loop(0, width // DOT_COLS, columns, 0)

        for sign, base, send, recv, g_send, g_recv in streams:
            place = me if sign == 1 else last - me
            chunk = step - place
            rows = pl.ds(pl.multiple_of(base + chunk * SUM_ROWS, SUM_ROWS), SUM_ROWS)
            inside = (chunk >= 0) & (chunk < chunks)
            nxt = me + sign
            prev = me - sign

            @pl.when(inside & (place > 0))
            def _():
                to_peer(total.at[rows], came.at[rows], send.at[chunk], recv.at[chunk], me).wait_recv()

                @pl.when(place < last)
                def _():
                    total[rows, :] = total[rows, :] + came[rows, :]

                @pl.when(place == last)
                def _():
                    update = (total[rows, :] + came[rows, :]).astype(jnp.bfloat16).astype(jnp.float32)
                    out_ref[rows, :] = (hid_ref[rows, :].astype(jnp.float32) + update).astype(jnp.bfloat16)
                    to_peer(out_ref.at[rows], out_ref.at[rows], g_send.at[chunk], g_recv.at[chunk], prev).start()

            @pl.when(inside & (place < last))
            def _():
                to_peer(total.at[rows], came.at[rows], send.at[chunk], recv.at[chunk], nxt).start()

        for sign, base, send, recv, g_send, g_recv in streams:
            place = me if sign == 1 else last - me
            chunk = step - last - (last - place)
            rows = pl.ds(pl.multiple_of(base + chunk * SUM_ROWS, SUM_ROWS), SUM_ROWS)
            prev = me - sign

            @pl.when((chunk >= 0) & (chunk < chunks) & (place < last))
            def _():
                to_peer(out_ref.at[rows], out_ref.at[rows], g_send.at[chunk], g_recv.at[chunk], me).wait_recv()

                @pl.when(place > 0)
                def _():
                    to_peer(out_ref.at[rows], out_ref.at[rows], g_send.at[chunk], g_recv.at[chunk], prev).start()
        return carry

    lax.fori_loop(0, chunks + 2 * last, tick, 0)

    def drain(chunk, carry):
        for sign, base, send, recv, g_send, g_recv in streams:
            place = me if sign == 1 else last - me
            rows = pl.ds(pl.multiple_of(base + chunk * SUM_ROWS, SUM_ROWS), SUM_ROWS)

            @pl.when(place < last)
            def _():
                to_peer(total.at[rows], came.at[rows], send.at[chunk], recv.at[chunk], me + sign).wait_send()

            @pl.when(place > 0)
            def _():
                to_peer(out_ref.at[rows], out_ref.at[rows], g_send.at[chunk], g_recv.at[chunk], me - sign).wait_send()
        return carry

    lax.fori_loop(0, chunks, drain, 0)
    sum_small(me, tp_size, part_ref, held, sm_send, sm_recv, small_ref)


def down_and_sum(act, w_down, hidden, small_part, tp_size):
    rows, width = hidden.shape
    chunks = rows // 2 // SUM_ROWS
    vmem = pl.BlockSpec(memory_space=pltpu.VMEM)
    return pl.pallas_call(
        lambda *refs: sum_kernel(tp_size, *refs),
        out_shape=(jax.ShapeDtypeStruct(hidden.shape, hidden.dtype), jax.ShapeDtypeStruct(small_part.shape, jnp.bfloat16)),
        in_specs=[vmem] * 4,
        out_specs=(vmem, vmem),
        scratch_shapes=[pltpu.VMEM((rows, width), jnp.float32), pltpu.VMEM((rows, width), jnp.float32), pltpu.VMEM((tp_size,) + small_part.shape, jnp.float32)] + [pltpu.SemaphoreType.DMA((chunks,))] * 8 + [pltpu.SemaphoreType.DMA((tp_size - 1,)), pltpu.SemaphoreType.DMA((tp_size,))],
        compiler_params=pltpu.CompilerParams(collective_id=1, has_side_effects=True, vmem_limit_bytes=VMEM_BYTES),
        cost_estimate=pl.CostEstimate(flops=150_000_000_000, bytes_accessed=rows * width * 10, transcendentals=0),
        name='down_sum',
    )(act, w_down, hidden, small_part)


def rms_norm(hidden, gain_vec):
    hid_f32 = hidden.astype(jnp.float32)
    inv_rms = lax.rsqrt(jnp.mean(hid_f32 * hid_f32, axis=-1, keepdims=True) + EPSILON)
    return (hid_f32 * inv_rms * gain_vec).astype(jnp.bfloat16)


def add_residual(hidden, update):
    return (hidden.astype(jnp.float32) + update.astype(jnp.float32)).astype(jnp.bfloat16)


def rope_tables(positions, head_dim):
    half_dim = head_dim // 2
    inv_freq = THETA ** (-jnp.arange(half_dim, dtype=jnp.float32) * 2.0 / head_dim)
    angles = positions.astype(jnp.float32)[:, None] * inv_freq[None, :]
    return jnp.cos(angles), jnp.sin(angles)


def apply_rope(values_in, cos_tab, sin_tab):
    half_dim = values_in.shape[-1] // 2
    lower_half = values_in[..., :half_dim]
    upper_half = values_in[..., half_dim:]
    cos_b = cos_tab[:, None, :]
    sin_b = sin_tab[:, None, :]
    return jnp.concatenate([lower_half * cos_b - upper_half * sin_b, upper_half * cos_b + lower_half * sin_b], axis=-1)


def swiglu(hidden, gain_vec, w_gu):
    normed = rms_norm(hidden, gain_vec)
    gate_up = jnp.einsum('sd,kfd->skf', normed, w_gu, preferred_element_type=jnp.float32)
    gate_val = gate_up[..., 0, :].astype(jnp.bfloat16).astype(jnp.float32)
    up_val = gate_up[..., 1, :].astype(jnp.bfloat16).astype(jnp.float32)
    return (jax.nn.silu(gate_val) * up_val).astype(jnp.bfloat16)


def prompt_attention(queries, keys_in, values_in, allowed):
    attn_scale = queries.shape[-1] ** -0.5
    scores = jnp.einsum('qhe,khe->hqk', queries, keys_in, preferred_element_type=jnp.float32) * attn_scale
    scores = jnp.where(allowed[None], scores, MASKED)
    prob_bf = jax.nn.softmax(scores, axis=-1).astype(jnp.bfloat16)
    return jnp.einsum('hqk,khe->qhe', prob_bf, values_in, preferred_element_type=jnp.float32).astype(jnp.bfloat16)


def decode_attention(queries, k_tok, v_tok, k_layer, v_layer, visible):
    attn_scale = queries.shape[-1] ** -0.5
    cache_scores = jnp.einsum('bhe,bthe->bht', queries, k_layer, preferred_element_type=jnp.float32) * attn_scale
    cache_scores = jnp.where(visible, cache_scores, MASKED)
    self_score = jnp.einsum('bhe,bhe->bh', queries, k_tok, preferred_element_type=jnp.float32) * attn_scale
    row_max = jnp.maximum(jnp.max(cache_scores, axis=-1), self_score)
    cache_exp = jnp.exp(cache_scores - row_max[..., None])
    self_exp = jnp.exp(self_score - row_max)
    denominator = jnp.sum(cache_exp, axis=-1) + self_exp
    cache_prob = (cache_exp / denominator[..., None]).astype(jnp.bfloat16)
    self_prob = (self_exp / denominator).astype(jnp.bfloat16).astype(jnp.float32)
    context = jnp.einsum('bht,bthe->bhe', cache_prob, v_layer, preferred_element_type=jnp.float32) + self_prob[..., None] * v_tok.astype(jnp.float32)
    return context.astype(jnp.bfloat16)


def run_layers(prompt, s_valid, w_qkv_pre, wo_full, w_gu_pre, w_down_pre, gains_pre, tokens, k_cache, v_cache, c_len, w_qkv_dec, w_out_dec, w_gu_dec, w_down_dec, gains_dec, partner_perm, tp_size):
    layers, row_count, cache_len, heads_loc, _, head_dim = k_cache.shape
    width = tokens.shape[1]
    seq_len = prompt.shape[0]
    k_local = k_cache.reshape(layers, row_count, cache_len, heads_loc, head_dim)
    v_local = v_cache.reshape(layers, row_count, cache_len, heads_loc, head_dim)
    wqkv_local = w_qkv_dec.reshape(layers, width, 3, heads_loc, head_dim)
    wout_local = w_out_dec.reshape(layers, heads_loc, head_dim, width)
    cos_dec, sin_dec = rope_tables(c_len, head_dim)
    cache_pos = jnp.arange(cache_len)
    visible = (cache_pos[None, :] < c_len[:, None])[:, None, :]
    write_at = (cache_pos[None, :] == c_len[:, None])[:, :, None, None]
    positions = jnp.arange(seq_len)
    cos_pre, sin_pre = rope_tables(positions, head_dim)
    allowed = (positions[None, :] <= positions[:, None]) & (positions[None, :] < s_valid[:, None])
    hidden = prompt
    installed, k_next, v_next = [], [], []
    for layer_idx in range(layers):
        normed = rms_norm(hidden, gains_pre[layer_idx, 0])
        qkv_out = jnp.einsum('sd,dkhe->skhe', normed, w_qkv_pre[layer_idx], preferred_element_type=jnp.float32)
        queries = apply_rope(qkv_out[:, 0], cos_pre, sin_pre).astype(jnp.bfloat16)
        keys_new = apply_rope(qkv_out[:, 1], cos_pre, sin_pre).astype(jnp.bfloat16)
        values_new = qkv_out[:, 2].astype(jnp.bfloat16)
        context = prompt_attention(queries, keys_new, values_new, allowed).reshape(seq_len, -1)

        normed_tok = rms_norm(tokens, gains_dec[layer_idx, 0])
        qkv_tok = jnp.einsum('bd,dkhe->bkhe', normed_tok, wqkv_local[layer_idx], preferred_element_type=jnp.float32)
        q_tok = apply_rope(qkv_tok[:, 0], cos_dec, sin_dec).astype(jnp.bfloat16)
        k_tok = apply_rope(qkv_tok[:, 1], cos_dec, sin_dec).astype(jnp.bfloat16)
        v_tok = qkv_tok[:, 2].astype(jnp.bfloat16)
        ctx_tok = decode_attention(q_tok, k_tok, v_tok, k_local[layer_idx], v_local[layer_idx], visible)
        part_tok = jnp.einsum('bhe,hed->bd', ctx_tok, wout_local[layer_idx], preferred_element_type=jnp.float32)
        k_next.append(jnp.where(write_at, k_tok[:, None], k_local[layer_idx]))
        v_next.append(jnp.where(write_at, v_tok[:, None], v_local[layer_idx]))

        ctx_full, attn_tok = gather_ctx(context, part_tok, tp_size)
        kv_new = lax.ppermute(jnp.stack([keys_new, values_new]), 'side', partner_perm)
        installed.append(lax.all_to_all(kv_new, 'tp', 2, 2, tiled=True))

        attn = jnp.einsum('zsf,zfd->sd', ctx_full, wo_full[layer_idx], preferred_element_type=jnp.float32)
        hidden = add_residual(hidden, attn.astype(jnp.bfloat16))
        act = swiglu(hidden, gains_pre[layer_idx, 1], w_gu_pre[layer_idx])
        tokens = add_residual(tokens, attn_tok)
        act_tok = swiglu(tokens, gains_dec[layer_idx, 1], w_gu_dec[layer_idx])
        mlp_tok = jnp.einsum('bf,fd->bd', act_tok, w_down_dec[layer_idx], preferred_element_type=jnp.float32)
        hidden, down_tok = down_and_sum(act, w_down_pre[layer_idx], hidden, mlp_tok, tp_size)
        tokens = add_residual(tokens, down_tok)
    k_new = jnp.stack(k_next).reshape(k_cache.shape)
    v_new = jnp.stack(v_next).reshape(v_cache.shape)
    return hidden, tokens, installed, k_new, v_new


def gather_wo(w_out, side_size, pair_size):
    layers, heads_loc, head_dim, width = w_out.shape
    rows = heads_loc * head_dim
    copies = side_size * pair_size
    part = rows // copies
    place = lax.axis_index('pair') * side_size + lax.axis_index('side')
    flat = w_out.reshape(layers, rows, width)
    mine = lax.dynamic_slice_in_dim(flat, place * part, part, axis=1)
    full = []
    for layer_idx in range(layers):
        everything = lax.all_gather(mine[layer_idx], ('tp', 'pair', 'side'), axis=0, tiled=True)
        full.append(everything.reshape(-1, rows, width))
    return full


def solution(mesh):
    tp_size = mesh.shape['tp']
    side_size = mesh.shape['side']
    pair_size = mesh.shape['pair']
    partner_perm = [(src_idx, (src_idx + side_size // 2) % side_size) for src_idx in range(side_size)]
    inst_axes = ('pair', 'side')
    rows_spec = P(inst_axes, None)
    vec_spec = P(inst_axes)
    cache_spec = P(None, inst_axes, None, None, 'tp', None)
    prompt_spec = P(None, inst_axes, None, 'tp', None)
    in_specs = (rows_spec, vec_spec, P(None, None, None, 'tp', None), P(None, 'tp', None, None), P(None, None, 'tp', None), P(None, 'tp', None), P(None, None, None), rows_spec, cache_spec, cache_spec, vec_spec, P(None, None, None, None, 'tp', None), P(None, None, 'tp', None, None), P(None, None, 'tp', None), P(None, 'tp', None), P(None, None, None))
    out_specs = (rows_spec, rows_spec, prompt_spec, prompt_spec, cache_spec, cache_spec)

    def device_fn(prompt_x, s_len, w_qkv_pre, w_out_pre, w_gu_pre, w_down_pre, gain_pre, dec_tokens, k_cache, v_cache, c_len, w_qkv_dec, w_out_dec, w_gu_dec, w_down_dec, gain_dec):
        wo_full = gather_wo(w_out_pre, side_size, pair_size)
        hidden, dec_out, installed, k_cache_new, v_cache_new = run_layers(prompt_x, s_len, w_qkv_pre, wo_full, w_gu_pre, w_down_pre, gain_pre, dec_tokens, k_cache, v_cache, c_len, w_qkv_dec, w_out_dec, w_gu_dec, w_down_dec, gain_dec, partner_perm, tp_size)
        prompt_kv = jnp.stack(installed, axis=1)[:, :, :, :, None, :]
        return hidden, dec_out, prompt_kv[0], prompt_kv[1], k_cache_new, v_cache_new

    return jax.shard_map(device_fn, mesh=mesh, in_specs=in_specs, out_specs=out_specs, check_vma=False)
```

```python
import jax
import jax.numpy as jnp
from jax import lax
from jax.experimental import pallas as pl
from jax.experimental.pallas import tpu as pltpu
from jax.sharding import PartitionSpec as P

EPSILON = 1e-6
THETA = 10000.0
MASKED = -1e30
CTX_ROWS = 128
SUM_ROWS = 32
DOT_ROWS = 128
DOT_COLS = 512
FF_COLS = 256
SUM_VMEM_BYTES = 63 * 1024 * 1024
VMEM_BYTES = 56 * 1024 * 1024
MESH = pl.DeviceIdType.MESH


def greet(me, tp_size):
    barrier = pltpu.get_barrier_semaphore()
    for off in range(1, tp_size):
        pl.semaphore_signal(barrier, inc=1, device_id={'tp': lax.rem(me + off, tp_size)}, device_id_type=MESH)
    pl.semaphore_wait(barrier, tp_size - 1)


def to_peer(src, dst, send_sem, recv_sem, peer):
    return pltpu.make_async_remote_copy(src_ref=src, dst_ref=dst, send_sem=send_sem, recv_sem=recv_sem, device_id={'tp': peer}, device_id_type=MESH)


def share_small(me, tp_size, part_ref, held, send_sems, recv_sems):
    for off in range(1, tp_size):
        peer = lax.rem(me + off, tp_size)
        to_peer(part_ref, held.at[me], send_sems.at[off - 1], recv_sems.at[me], peer).start()


def sum_small(me, tp_size, part_ref, held, send_sems, recv_sems, out_ref):
    for off in range(1, tp_size):
        peer = lax.rem(me + off, tp_size)
        copy = to_peer(part_ref, held.at[peer], send_sems.at[off - 1], recv_sems.at[peer], peer)
        copy.wait_send()
        copy.wait_recv()
    held[me] = part_ref[...]
    total = held[0]
    for idx in range(1, tp_size):
        total = total + held[idx]
    out_ref[...] = total.astype(out_ref.dtype)


def ctx_kernel(tp_size, ctx_ref, part_ref, full_ref, small_ref, held, up_send, up_recv, dn_send, dn_recv, sm_send, sm_recv):
    me = lax.axis_index('tp')
    last = tp_size - 1
    chunks = ctx_ref.shape[0] // CTX_ROWS
    greet(me, tp_size)
    share_small(me, tp_size, part_ref, held, sm_send, sm_recv)

    def rows_of(chunk):
        return pl.ds(pl.multiple_of(chunk * CTX_ROWS, CTX_ROWS), CTX_ROWS)

    def tick(step, carry):
        for back in range(tp_size):
            chunk = step - back
            inside = (chunk >= 0) & (chunk < chunks)
            for sign, send, recv in ((1, up_send, up_recv), (-1, dn_send, dn_recv)):
                shard = me - sign * back
                peer = me + sign
                has = inside & (shard >= 0) & (shard <= last)
                more = has & (peer >= 0) & (peer <= last)
                rows = rows_of(chunk)
                if back == 0:
                    @pl.when(more)
                    def _():
                        to_peer(ctx_ref.at[rows], full_ref.at[me, rows], send.at[0, chunk], recv.at[0, chunk], peer).start()
                else:
                    @pl.when(has)
                    def _():
                        to_peer(ctx_ref.at[rows], full_ref.at[shard, rows], send.at[back - 1, chunk], recv.at[back - 1, chunk], me).wait_recv()
                    if back < last:
                        @pl.when(more)
                        def _():
                            to_peer(full_ref.at[shard, rows], full_ref.at[shard, rows], send.at[back, chunk], recv.at[back, chunk], peer).start()
        return carry

    lax.fori_loop(0, chunks + last, tick, 0)
    full_ref[me] = ctx_ref[...]

    def drain(chunk, carry):
        for back in range(last):
            for sign, send, recv in ((1, up_send, up_recv), (-1, dn_send, dn_recv)):
                shard = me - sign * back
                peer = me + sign

                @pl.when((shard >= 0) & (shard <= last) & (peer >= 0) & (peer <= last))
                def _():
                    to_peer(ctx_ref.at[rows_of(chunk)], full_ref.at[me, rows_of(chunk)], send.at[back, chunk], recv.at[back, chunk], peer).wait_send()
        return carry

    lax.fori_loop(0, chunks, drain, 0)
    sum_small(me, tp_size, part_ref, held, sm_send, sm_recv, small_ref)


def gather_ctx(ctx, small_part, tp_size):
    rows, width = ctx.shape
    chunks = rows // CTX_ROWS
    last = tp_size - 1
    vmem = pl.BlockSpec(memory_space=pltpu.VMEM)
    return pl.pallas_call(
        lambda *refs: ctx_kernel(tp_size, *refs),
        out_shape=(jax.ShapeDtypeStruct((tp_size, rows, width), ctx.dtype), jax.ShapeDtypeStruct(small_part.shape, jnp.bfloat16)),
        in_specs=[vmem, vmem],
        out_specs=(vmem, vmem),
        scratch_shapes=[pltpu.VMEM((tp_size,) + small_part.shape, jnp.float32)] + [pltpu.SemaphoreType.DMA((last, chunks))] * 4 + [pltpu.SemaphoreType.DMA((last,)), pltpu.SemaphoreType.DMA((tp_size,))],
        compiler_params=pltpu.CompilerParams(collective_id=0, has_side_effects=True, vmem_limit_bytes=VMEM_BYTES),
        cost_estimate=pl.CostEstimate(flops=70_000_000_000, bytes_accessed=rows * width * 10, transcendentals=0),
        name='ctx_gather',
    )(ctx, small_part)


def sum_kernel(layer, tp_size, ctx_hbm, hid_hbm, wo_hbm, gu_hbm, wd_hbm, gain_ref, part_ref, out_ref, small_ref, ctx_ref, hid_ref, wo_ref, gu_ref, wd_ref, norm_ref, act_ref, total, came, held, in_sems, up_send, up_recv, dn_send, dn_recv, gu_send, gu_recv, gd_send, gd_recv, sm_send, sm_recv):
    me = lax.axis_index('tp')
    last = tp_size - 1
    half = hid_ref.shape[0] // 2
    chunks = half // SUM_ROWS
    per_dot = DOT_ROWS // SUM_ROWS
    width = hid_ref.shape[1]
    ff_loc = wd_ref.shape[0]
    shard = ctx_ref.shape[2]
    loads = [
        pltpu.make_async_copy(ctx_hbm, ctx_ref, in_sems.at[0]),
        pltpu.make_async_copy(hid_hbm, hid_ref, in_sems.at[1]),
        pltpu.make_async_copy(wo_hbm, wo_ref, in_sems.at[2]),
        pltpu.make_async_copy(gu_hbm.at[layer], gu_ref, in_sems.at[3]),
        pltpu.make_async_copy(wd_hbm.at[layer], wd_ref, in_sems.at[4]),
    ]
    for load in loads:
        load.start()
    greet(me, tp_size)
    share_small(me, tp_size, part_ref, held, sm_send, sm_recv)
    streams = ((1, half, up_send, up_recv, gu_send, gu_recv), (-1, 0, dn_send, dn_recv, gd_send, gd_recv))
    full_ff = ff_loc // FF_COLS
    rest = ff_loc - full_ff * FF_COLS
    first_part = (full_ff + 1) // 2

    def activate(start, size):
        normed = norm_ref[...]
        contract = (((1,), (1,)), ((), ()))
        gate = lax.dot_general(normed, gu_ref[0, pl.ds(start, size), :], contract, preferred_element_type=jnp.float32)
        up = lax.dot_general(normed, gu_ref[1, pl.ds(start, size), :], contract, preferred_element_type=jnp.float32)
        gate = gate.astype(jnp.bfloat16).astype(jnp.float32)
        up = up.astype(jnp.bfloat16).astype(jnp.float32)
        act_ref[:, pl.ds(start, size)] = (jax.nn.silu(gate) * up).astype(jnp.bfloat16)

    def tick(time, carry):
        step = time - per_dot
        stage = lax.rem(time, per_dot)
        block = time // per_dot
        working = time < chunks
        block_rows = [pl.ds(pl.multiple_of(base + block * DOT_ROWS, DOT_ROWS), DOT_ROWS) for base in (half, 0)]

        @pl.when(time == 0)
        def _():
            for load in loads[:3]:
                load.wait()

        @pl.when(time == 1)
        def _():
            loads[3].wait()

        @pl.when(time == 3)
        def _():
            loads[4].wait()

        @pl.when(working & (stage == 0))
        def _():
            def columns(idx, inner):
                cols = pl.ds(pl.multiple_of(idx * DOT_COLS, DOT_COLS), DOT_COLS)
                attn = None
                for src in range(tp_size):
                    both = jnp.concatenate([ctx_ref[src, rows, :] for rows in block_rows], axis=0)
                    term = jnp.dot(both, wo_ref[src * shard:(src + 1) * shard, cols], preferred_element_type=jnp.float32)
                    attn = term if attn is None else attn + term
                attn = attn.astype(jnp.bfloat16).astype(jnp.float32)
                for idx_rows, rows in enumerate(block_rows):
                    old = hid_ref[rows, cols].astype(jnp.float32)
                    hid_ref[rows, cols] = (old + attn[idx_rows * DOT_ROWS:(idx_rows + 1) * DOT_ROWS]).astype(jnp.bfloat16)
                return inner

            lax.fori_loop(0, width // DOT_COLS, columns, 0)
            for idx_rows, rows in enumerate(block_rows):
                for sub in range(0, DOT_ROWS, 32):
                    piece = pl.ds(pl.multiple_of(rows.start + sub, 32), 32)
                    hid = hid_ref[piece, :].astype(jnp.float32)
                    inv_rms = lax.rsqrt(jnp.mean(hid * hid, axis=-1, keepdims=True) + EPSILON)
                    norm_ref[idx_rows * DOT_ROWS + sub:idx_rows * DOT_ROWS + sub + 32, :] = (hid * inv_rms * gain_ref[...]).astype(jnp.bfloat16)

        @pl.when(working & ((stage == 1) | (stage == 2)))
        def _():
            low = (stage - 1) * first_part
            high = first_part + (stage - 1) * (full_ff - first_part)

            def features(idx, inner):
                activate(pl.multiple_of(idx * FF_COLS, FF_COLS), FF_COLS)
                return inner

            lax.fori_loop(low, high, features, 0)

        if rest:
            @pl.when(working & (stage == 2))
            def _():
                activate(full_ff * FF_COLS, rest)

        @pl.when(working & (stage == 3))
        def _():
            def columns(idx, inner):
                cols = pl.ds(pl.multiple_of(idx * DOT_COLS, DOT_COLS), DOT_COLS)
                part = jnp.dot(act_ref[...], wd_ref[:, cols], preferred_element_type=jnp.float32)
                for idx_rows, rows in enumerate(block_rows):
                    total[rows, cols] = part[idx_rows * DOT_ROWS:(idx_rows + 1) * DOT_ROWS]
                return inner

            lax.fori_loop(0, width // DOT_COLS, columns, 0)

        for sign, base, send, recv, g_send, g_recv in streams:
            place = me if sign == 1 else last - me
            chunk = step - place
            rows = pl.ds(pl.multiple_of(base + chunk * SUM_ROWS, SUM_ROWS), SUM_ROWS)
            inside = (chunk >= 0) & (chunk < chunks)
            nxt = me + sign
            prev = me - sign

            @pl.when(inside & (place > 0))
            def _():
                to_peer(total.at[rows], came.at[rows], send.at[chunk], recv.at[chunk], me).wait_recv()

                @pl.when(place < last)
                def _():
                    total[rows, :] = total[rows, :] + came[rows, :]

                @pl.when(place == last)
                def _():
                    update = (total[rows, :] + came[rows, :]).astype(jnp.bfloat16).astype(jnp.float32)
                    out_ref[rows, :] = (hid_ref[rows, :].astype(jnp.float32) + update).astype(jnp.bfloat16)
                    to_peer(out_ref.at[rows], out_ref.at[rows], g_send.at[chunk], g_recv.at[chunk], prev).start()

            @pl.when(inside & (place < last))
            def _():
                to_peer(total.at[rows], came.at[rows], send.at[chunk], recv.at[chunk], nxt).start()

        for sign, base, send, recv, g_send, g_recv in streams:
            place = me if sign == 1 else last - me
            chunk = step - last - (last - place)
            rows = pl.ds(pl.multiple_of(base + chunk * SUM_ROWS, SUM_ROWS), SUM_ROWS)
            prev = me - sign

            @pl.when((chunk >= 0) & (chunk < chunks) & (place < last))
            def _():
                to_peer(out_ref.at[rows], out_ref.at[rows], g_send.at[chunk], g_recv.at[chunk], me).wait_recv()

                @pl.when(place > 0)
                def _():
                    to_peer(out_ref.at[rows], out_ref.at[rows], g_send.at[chunk], g_recv.at[chunk], prev).start()
        return carry

    lax.fori_loop(0, per_dot + chunks + 2 * last, tick, 0)

    def drain(chunk, carry):
        for sign, base, send, recv, g_send, g_recv in streams:
            place = me if sign == 1 else last - me
            rows = pl.ds(pl.multiple_of(base + chunk * SUM_ROWS, SUM_ROWS), SUM_ROWS)

            @pl.when(place < last)
            def _():
                to_peer(total.at[rows], came.at[rows], send.at[chunk], recv.at[chunk], me + sign).wait_send()

            @pl.when(place > 0)
            def _():
                to_peer(out_ref.at[rows], out_ref.at[rows], g_send.at[chunk], g_recv.at[chunk], me - sign).wait_send()
        return carry

    lax.fori_loop(0, chunks, drain, 0)
    sum_small(me, tp_size, part_ref, held, sm_send, sm_recv, small_ref)


def mlp_and_sum(layer, ctx_full, hidden, wo_full, w_gu, w_down, gain, small_part, tp_size):
    rows, width = hidden.shape
    chunks = rows // 2 // SUM_ROWS
    ff_loc = w_down.shape[1]
    vmem = pl.BlockSpec(memory_space=pltpu.VMEM)
    hbm = pl.BlockSpec(memory_space=pl.ANY)
    bf16 = jnp.bfloat16
    return pl.pallas_call(
        lambda *refs: sum_kernel(layer, tp_size, *refs),
        out_shape=(jax.ShapeDtypeStruct(hidden.shape, hidden.dtype), jax.ShapeDtypeStruct(small_part.shape, bf16)),
        in_specs=[hbm] * 5 + [vmem] * 2,
        out_specs=(vmem, vmem),
        scratch_shapes=[
            pltpu.VMEM(ctx_full.shape, bf16),
            pltpu.VMEM((rows, width), bf16),
            pltpu.VMEM(wo_full.shape, bf16),
            pltpu.VMEM((2, ff_loc, width), bf16),
            pltpu.VMEM((ff_loc, width), bf16),
            pltpu.VMEM((2 * DOT_ROWS, width), bf16),
            pltpu.VMEM((2 * DOT_ROWS, ff_loc), bf16),
            pltpu.VMEM((rows, width), jnp.float32),
            pltpu.VMEM((rows, width), jnp.float32),
            pltpu.VMEM((tp_size,) + small_part.shape, jnp.float32),
            pltpu.SemaphoreType.DMA((5,)),
        ] + [pltpu.SemaphoreType.DMA((chunks,))] * 8 + [pltpu.SemaphoreType.DMA((tp_size - 1,)), pltpu.SemaphoreType.DMA((tp_size,))],
        compiler_params=pltpu.CompilerParams(collective_id=1 + layer, has_side_effects=True, vmem_limit_bytes=SUM_VMEM_BYTES),
        cost_estimate=pl.CostEstimate(flops=160_000_000_000, bytes_accessed=rows * width * 20, transcendentals=0),
        name='mlp_sum',
    )(ctx_full, hidden, wo_full, w_gu, w_down, gain, small_part)


def rms_norm(hidden, gain_vec):
    hid_f32 = hidden.astype(jnp.float32)
    inv_rms = lax.rsqrt(jnp.mean(hid_f32 * hid_f32, axis=-1, keepdims=True) + EPSILON)
    return (hid_f32 * inv_rms * gain_vec).astype(jnp.bfloat16)


def add_residual(hidden, update):
    return (hidden.astype(jnp.float32) + update.astype(jnp.float32)).astype(jnp.bfloat16)


def rope_tables(positions, head_dim):
    half_dim = head_dim // 2
    inv_freq = THETA ** (-jnp.arange(half_dim, dtype=jnp.float32) * 2.0 / head_dim)
    angles = positions.astype(jnp.float32)[:, None] * inv_freq[None, :]
    return jnp.cos(angles), jnp.sin(angles)


def apply_rope(values_in, cos_tab, sin_tab):
    half_dim = values_in.shape[-1] // 2
    lower_half = values_in[..., :half_dim]
    upper_half = values_in[..., half_dim:]
    cos_b = cos_tab[:, None, :]
    sin_b = sin_tab[:, None, :]
    return jnp.concatenate([lower_half * cos_b - upper_half * sin_b, upper_half * cos_b + lower_half * sin_b], axis=-1)


def swiglu(hidden, gain_vec, w_gu):
    normed = rms_norm(hidden, gain_vec)
    gate_up = jnp.einsum('sd,kfd->skf', normed, w_gu, preferred_element_type=jnp.float32)
    gate_val = gate_up[..., 0, :].astype(jnp.bfloat16).astype(jnp.float32)
    up_val = gate_up[..., 1, :].astype(jnp.bfloat16).astype(jnp.float32)
    return (jax.nn.silu(gate_val) * up_val).astype(jnp.bfloat16)


def prompt_attention(queries, keys_in, values_in, allowed):
    attn_scale = queries.shape[-1] ** -0.5
    scores = jnp.einsum('qhe,khe->hqk', queries, keys_in, preferred_element_type=jnp.float32) * attn_scale
    scores = jnp.where(allowed[None], scores, MASKED)
    prob_bf = jax.nn.softmax(scores, axis=-1).astype(jnp.bfloat16)
    return jnp.einsum('hqk,khe->qhe', prob_bf, values_in, preferred_element_type=jnp.float32).astype(jnp.bfloat16)


def decode_attention(queries, k_tok, v_tok, k_layer, v_layer, visible):
    attn_scale = queries.shape[-1] ** -0.5
    cache_scores = jnp.einsum('bhe,bthe->bht', queries, k_layer, preferred_element_type=jnp.float32) * attn_scale
    cache_scores = jnp.where(visible, cache_scores, MASKED)
    self_score = jnp.einsum('bhe,bhe->bh', queries, k_tok, preferred_element_type=jnp.float32) * attn_scale
    row_max = jnp.maximum(jnp.max(cache_scores, axis=-1), self_score)
    cache_exp = jnp.exp(cache_scores - row_max[..., None])
    self_exp = jnp.exp(self_score - row_max)
    denominator = jnp.sum(cache_exp, axis=-1) + self_exp
    cache_prob = (cache_exp / denominator[..., None]).astype(jnp.bfloat16)
    self_prob = (self_exp / denominator).astype(jnp.bfloat16).astype(jnp.float32)
    context = jnp.einsum('bht,bthe->bhe', cache_prob, v_layer, preferred_element_type=jnp.float32) + self_prob[..., None] * v_tok.astype(jnp.float32)
    return context.astype(jnp.bfloat16)


def run_layers(prompt, s_valid, w_qkv_pre, wo_parts, w_gu_pre, w_down_pre, gains_pre, tokens, k_cache, v_cache, c_len, w_qkv_dec, w_out_dec, w_gu_dec, w_down_dec, gains_dec, partner_perm, tp_size):
    layers, row_count, cache_len, heads_loc, _, head_dim = k_cache.shape
    width = tokens.shape[1]
    seq_len = prompt.shape[0]
    k_local = k_cache.reshape(layers, row_count, cache_len, heads_loc, head_dim)
    v_local = v_cache.reshape(layers, row_count, cache_len, heads_loc, head_dim)
    wqkv_local = w_qkv_dec.reshape(layers, width, 3, heads_loc, head_dim)
    wout_local = w_out_dec.reshape(layers, heads_loc, head_dim, width)
    cos_dec, sin_dec = rope_tables(c_len, head_dim)
    cache_pos = jnp.arange(cache_len)
    visible = (cache_pos[None, :] < c_len[:, None])[:, None, :]
    write_at = (cache_pos[None, :] == c_len[:, None])[:, :, None, None]
    positions = jnp.arange(seq_len)
    cos_pre, sin_pre = rope_tables(positions, head_dim)
    allowed = (positions[None, :] <= positions[:, None]) & (positions[None, :] < s_valid[:, None])
    wqkv_flat = w_qkv_pre.reshape(layers, width, -1)
    hidden = prompt
    installed, k_next, v_next = [], [], []
    for layer_idx in range(layers):
        normed = rms_norm(hidden, gains_pre[layer_idx, 0])
        qkv_out = jnp.dot(normed, wqkv_flat[layer_idx], preferred_element_type=jnp.float32).reshape(seq_len, 3, heads_loc, head_dim)
        queries = apply_rope(qkv_out[:, 0], cos_pre, sin_pre).astype(jnp.bfloat16)
        keys_new = apply_rope(qkv_out[:, 1], cos_pre, sin_pre).astype(jnp.bfloat16)
        values_new = qkv_out[:, 2].astype(jnp.bfloat16)
        context = prompt_attention(queries, keys_new, values_new, allowed).reshape(seq_len, -1)

        normed_tok = rms_norm(tokens, gains_dec[layer_idx, 0])
        qkv_tok = jnp.einsum('bd,dkhe->bkhe', normed_tok, wqkv_local[layer_idx], preferred_element_type=jnp.float32)
        q_tok = apply_rope(qkv_tok[:, 0], cos_dec, sin_dec).astype(jnp.bfloat16)
        k_tok = apply_rope(qkv_tok[:, 1], cos_dec, sin_dec).astype(jnp.bfloat16)
        v_tok = qkv_tok[:, 2].astype(jnp.bfloat16)
        ctx_tok = decode_attention(q_tok, k_tok, v_tok, k_local[layer_idx], v_local[layer_idx], visible)
        part_tok = jnp.einsum('bhe,hed->bd', ctx_tok, wout_local[layer_idx], preferred_element_type=jnp.float32)
        k_next.append(jnp.where(write_at, k_tok[:, None], k_local[layer_idx]))
        v_next.append(jnp.where(write_at, v_tok[:, None], v_local[layer_idx]))

        ctx_full, attn_tok = gather_ctx(context, part_tok, tp_size)
        kv_new = lax.all_to_all(jnp.stack([keys_new, values_new]), 'tp', 2, 2, tiled=True)
        installed.append(lax.ppermute(kv_new, 'side', partner_perm))

        if layer_idx == 0:
            wo_full = gather_wo(wo_parts[0])
        else:
            wo_full = gather_wo(wo_next)
        tokens = add_residual(tokens, attn_tok)
        act_tok = swiglu(tokens, gains_dec[layer_idx, 1], w_gu_dec[layer_idx])
        mlp_tok = jnp.einsum('bf,fd->bd', act_tok, w_down_dec[layer_idx], preferred_element_type=jnp.float32)
        hidden, down_tok = mlp_and_sum(layer_idx, ctx_full, hidden, wo_full, w_gu_pre, w_down_pre, gains_pre[layer_idx, 1][None], mlp_tok, tp_size)
        if layer_idx + 1 < layers:
            wo_next, down_tok = lax.optimization_barrier((wo_parts[layer_idx + 1], down_tok))
        tokens = add_residual(tokens, down_tok)
    k_new = jnp.stack(k_next).reshape(k_cache.shape)
    v_new = jnp.stack(v_next).reshape(v_cache.shape)
    return hidden, tokens, installed, k_new, v_new


def parts_of_wo(w_out, side_size, pair_size):
    layers, heads_loc, head_dim, width = w_out.shape
    rows = heads_loc * head_dim
    part = rows // (side_size * pair_size)
    place = lax.axis_index('pair') * side_size + lax.axis_index('side')
    flat = w_out.reshape(layers, rows, width)
    return [lax.dynamic_slice(flat, (layer_idx, place * part, 0), (1, part, width))[0] for layer_idx in range(layers)]


def gather_wo(part):
    return lax.all_gather(part, ('tp', 'pair', 'side'), axis=0, tiled=True)


def solution(mesh):
    tp_size = mesh.shape['tp']
    side_size = mesh.shape['side']
    pair_size = mesh.shape['pair']
    partner_perm = [(src_idx, (src_idx + side_size // 2) % side_size) for src_idx in range(side_size)]
    inst_axes = ('pair', 'side')
    rows_spec = P(inst_axes, None)
    vec_spec = P(inst_axes)
    cache_spec = P(None, inst_axes, None, None, 'tp', None)
    prompt_spec = P(None, inst_axes, None, 'tp', None)
    in_specs = (rows_spec, vec_spec, P(None, None, None, 'tp', None), P(None, 'tp', None, None), P(None, None, 'tp', None), P(None, 'tp', None), P(None, None, None), rows_spec, cache_spec, cache_spec, vec_spec, P(None, None, None, None, 'tp', None), P(None, None, 'tp', None, None), P(None, None, 'tp', None), P(None, 'tp', None), P(None, None, None))
    out_specs = (rows_spec, rows_spec, prompt_spec, prompt_spec, cache_spec, cache_spec)

    def device_fn(prompt_x, s_len, w_qkv_pre, w_out_pre, w_gu_pre, w_down_pre, gain_pre, dec_tokens, k_cache, v_cache, c_len, w_qkv_dec, w_out_dec, w_gu_dec, w_down_dec, gain_dec):
        wo_parts = parts_of_wo(w_out_pre, side_size, pair_size)
        hidden, dec_out, installed, k_cache_new, v_cache_new = run_layers(prompt_x, s_len, w_qkv_pre, wo_parts, w_gu_pre, w_down_pre, gain_pre, dec_tokens, k_cache, v_cache, c_len, w_qkv_dec, w_out_dec, w_gu_dec, w_down_dec, gain_dec, partner_perm, tp_size)
        prompt_kv = jnp.stack(installed, axis=1)[:, :, :, :, None, :]
        return hidden, dec_out, prompt_kv[0], prompt_kv[1], k_cache_new, v_cache_new

    return jax.shard_map(device_fn, mesh=mesh, in_specs=in_specs, out_specs=out_specs, check_vma=False)
```

```python
import jax
import jax.numpy as jnp
from jax import lax
from jax.experimental import pallas as pl
from jax.experimental.pallas import tpu as pltpu
from jax.sharding import PartitionSpec as P

EPSILON = 1e-6
THETA = 10000.0
MASKED = -1e30
CTX_ROWS = 128
SUM_ROWS = 16
DOT_ROWS = 128
DOT_COLS = 512
STAGES = 4
FF_COLS = 256
SUM_VMEM_BYTES = 63 * 1024 * 1024
VMEM_BYTES = 56 * 1024 * 1024
MESH = pl.DeviceIdType.MESH


def greet(me, tp_size):
    barrier = pltpu.get_barrier_semaphore()
    for off in range(1, tp_size):
        pl.semaphore_signal(barrier, inc=1, device_id={'tp': lax.rem(me + off, tp_size)}, device_id_type=MESH)
    pl.semaphore_wait(barrier, tp_size - 1)


def to_peer(src, dst, send_sem, recv_sem, peer):
    return pltpu.make_async_remote_copy(src_ref=src, dst_ref=dst, send_sem=send_sem, recv_sem=recv_sem, device_id={'tp': peer}, device_id_type=MESH)


def share_small(me, tp_size, part_ref, held, send_sems, recv_sems):
    for off in range(1, tp_size):
        peer = lax.rem(me + off, tp_size)
        to_peer(part_ref, held.at[me], send_sems.at[off - 1], recv_sems.at[me], peer).start()


def sum_small(me, tp_size, part_ref, held, send_sems, recv_sems, out_ref):
    for off in range(1, tp_size):
        peer = lax.rem(me + off, tp_size)
        copy = to_peer(part_ref, held.at[peer], send_sems.at[off - 1], recv_sems.at[peer], peer)
        copy.wait_send()
        copy.wait_recv()
    held[me] = part_ref[...]
    total = held[0]
    for idx in range(1, tp_size):
        total = total + held[idx]
    out_ref[...] = total.astype(out_ref.dtype)


def ctx_kernel(tp_size, ctx_ref, part_ref, full_ref, small_ref, held, up_send, up_recv, dn_send, dn_recv, sm_send, sm_recv):
    me = lax.axis_index('tp')
    last = tp_size - 1
    chunks = ctx_ref.shape[0] // CTX_ROWS
    greet(me, tp_size)
    share_small(me, tp_size, part_ref, held, sm_send, sm_recv)

    def rows_of(chunk):
        return pl.ds(pl.multiple_of(chunk * CTX_ROWS, CTX_ROWS), CTX_ROWS)

    def tick(step, carry):
        for back in range(tp_size):
            chunk = step - back
            inside = (chunk >= 0) & (chunk < chunks)
            for sign, send, recv in ((1, up_send, up_recv), (-1, dn_send, dn_recv)):
                shard = me - sign * back
                peer = me + sign
                has = inside & (shard >= 0) & (shard <= last)
                more = has & (peer >= 0) & (peer <= last)
                rows = rows_of(chunk)
                if back == 0:
                    @pl.when(more)
                    def _():
                        to_peer(ctx_ref.at[rows], full_ref.at[me, rows], send.at[0, chunk], recv.at[0, chunk], peer).start()
                else:
                    @pl.when(has)
                    def _():
                        to_peer(ctx_ref.at[rows], full_ref.at[shard, rows], send.at[back - 1, chunk], recv.at[back - 1, chunk], me).wait_recv()
                    if back < last:
                        @pl.when(more)
                        def _():
                            to_peer(full_ref.at[shard, rows], full_ref.at[shard, rows], send.at[back, chunk], recv.at[back, chunk], peer).start()
        return carry

    lax.fori_loop(0, chunks + last, tick, 0)
    full_ref[me] = ctx_ref[...]

    def drain(chunk, carry):
        for back in range(last):
            for sign, send, recv in ((1, up_send, up_recv), (-1, dn_send, dn_recv)):
                shard = me - sign * back
                peer = me + sign

                @pl.when((shard >= 0) & (shard <= last) & (peer >= 0) & (peer <= last))
                def _():
                    to_peer(ctx_ref.at[rows_of(chunk)], full_ref.at[me, rows_of(chunk)], send.at[back, chunk], recv.at[back, chunk], peer).wait_send()
        return carry

    lax.fori_loop(0, chunks, drain, 0)
    sum_small(me, tp_size, part_ref, held, sm_send, sm_recv, small_ref)


def gather_ctx(ctx, small_part, tp_size):
    rows, width = ctx.shape
    chunks = rows // CTX_ROWS
    last = tp_size - 1
    vmem = pl.BlockSpec(memory_space=pltpu.VMEM)
    return pl.pallas_call(
        lambda *refs: ctx_kernel(tp_size, *refs),
        out_shape=(jax.ShapeDtypeStruct((tp_size, rows, width), ctx.dtype), jax.ShapeDtypeStruct(small_part.shape, jnp.bfloat16)),
        in_specs=[vmem, vmem],
        out_specs=(vmem, vmem),
        scratch_shapes=[pltpu.VMEM((tp_size,) + small_part.shape, jnp.float32)] + [pltpu.SemaphoreType.DMA((last, chunks))] * 4 + [pltpu.SemaphoreType.DMA((last,)), pltpu.SemaphoreType.DMA((tp_size,))],
        compiler_params=pltpu.CompilerParams(collective_id=0, has_side_effects=True, vmem_limit_bytes=VMEM_BYTES),
        cost_estimate=pl.CostEstimate(flops=70_000_000_000, bytes_accessed=rows * width * 10, transcendentals=0),
        name='ctx_gather',
    )(ctx, small_part)


def sum_kernel(layer, tp_size, ctx_hbm, hid_hbm, wo_hbm, gu_hbm, wd_hbm, gain_ref, part_ref, out_ref, small_ref, ctx_ref, hid_ref, wo_ref, gu_ref, wd_ref, norm_ref, act_ref, total, came, held, in_sems, up_send, up_recv, dn_send, dn_recv, gu_send, gu_recv, gd_send, gd_recv, sm_send, sm_recv):
    me = lax.axis_index('tp')
    last = tp_size - 1
    half = hid_ref.shape[0] // 2
    chunks = half // SUM_ROWS
    per_dot = DOT_ROWS // SUM_ROWS
    width = hid_ref.shape[1]
    ff_loc = wd_ref.shape[0]
    shard = ctx_ref.shape[2]
    loads = [
        pltpu.make_async_copy(ctx_hbm, ctx_ref, in_sems.at[0]),
        pltpu.make_async_copy(hid_hbm, hid_ref, in_sems.at[1]),
        pltpu.make_async_copy(gu_hbm.at[layer], gu_ref, in_sems.at[2]),
        pltpu.make_async_copy(wd_hbm.at[layer], wd_ref, in_sems.at[3]),
    ]
    weight_loads = [pltpu.make_async_copy(wo_hbm.at[:, src], wo_ref.at[src], in_sems.at[4 + src]) for src in range(tp_size)]
    loads = loads[:2] + weight_loads + loads[2:]
    for load in loads:
        load.start()
    greet(me, tp_size)
    share_small(me, tp_size, part_ref, held, sm_send, sm_recv)
    streams = ((1, half, up_send, up_recv, gu_send, gu_recv), (-1, 0, dn_send, dn_recv, gd_send, gd_recv))
    full_ff = ff_loc // FF_COLS
    rest = ff_loc - full_ff * FF_COLS
    first_part = (full_ff + 1) // 2

    def activate(start, size):
        normed = norm_ref[...]
        contract = (((1,), (1,)), ((), ()))
        gate = lax.dot_general(normed, gu_ref[0, pl.ds(start, size), :], contract, preferred_element_type=jnp.float32)
        up = lax.dot_general(normed, gu_ref[1, pl.ds(start, size), :], contract, preferred_element_type=jnp.float32)
        gate = gate.astype(jnp.bfloat16).astype(jnp.float32)
        up = up.astype(jnp.bfloat16).astype(jnp.float32)
        act_ref[:, pl.ds(start, size)] = (jax.nn.silu(gate) * up).astype(jnp.bfloat16)

    def tick(time, carry):
        step = time - per_dot
        pace = per_dot // STAGES
        on_beat = lax.rem(time, pace) == 0
        stage = lax.rem(time, per_dot) // pace
        block = time // per_dot
        working = (time < chunks) & on_beat
        block_rows = [pl.ds(pl.multiple_of(base + block * DOT_ROWS, DOT_ROWS), DOT_ROWS) for base in (half, 0)]

        @pl.when(time == 0)
        def _():
            for load in loads[:-2]:
                load.wait()

        @pl.when(time == pace)
        def _():
            loads[-2].wait()

        @pl.when(time == 3 * pace)
        def _():
            loads[-1].wait()

        @pl.when(working & (stage == 0))
        def _():
            def columns(idx, inner):
                cols = pl.ds(pl.multiple_of(idx * DOT_COLS, DOT_COLS), DOT_COLS)
                attn = None
                for src in range(tp_size):
                    both = jnp.concatenate([ctx_ref[src, rows, :] for rows in block_rows], axis=0)
                    term = jnp.dot(both, wo_ref[src, :, :, cols].reshape(shard, DOT_COLS), preferred_element_type=jnp.float32)
                    attn = term if attn is None else attn + term
                attn = attn.astype(jnp.bfloat16).astype(jnp.float32)
                for idx_rows, rows in enumerate(block_rows):
                    old = hid_ref[rows, cols].astype(jnp.float32)
                    hid_ref[rows, cols] = (old + attn[idx_rows * DOT_ROWS:(idx_rows + 1) * DOT_ROWS]).astype(jnp.bfloat16)
                return inner

            lax.fori_loop(0, width // DOT_COLS, columns, 0)
            for idx_rows, rows in enumerate(block_rows):
                for sub in range(0, DOT_ROWS, 32):
                    piece = pl.ds(pl.multiple_of(rows.start + sub, 32), 32)
                    hid = hid_ref[piece, :].astype(jnp.float32)
                    inv_rms = lax.rsqrt(jnp.mean(hid * hid, axis=-1, keepdims=True) + EPSILON)
                    norm_ref[idx_rows * DOT_ROWS + sub:idx_rows * DOT_ROWS + sub + 32, :] = (hid * inv_rms * gain_ref[...]).astype(jnp.bfloat16)

        @pl.when(working & ((stage == 1) | (stage == 2)))
        def _():
            low = (stage - 1) * first_part
            high = first_part + (stage - 1) * (full_ff - first_part)

            def features(idx, inner):
                activate(pl.multiple_of(idx * FF_COLS, FF_COLS), FF_COLS)
                return inner

            lax.fori_loop(low, high, features, 0)

        if rest:
            @pl.when(working & (stage == 2))
            def _():
                activate(full_ff * FF_COLS, rest)

        @pl.when(working & (stage == 3))
        def _():
            def columns(idx, inner):
                cols = pl.ds(pl.multiple_of(idx * DOT_COLS, DOT_COLS), DOT_COLS)
                part = jnp.dot(act_ref[...], wd_ref[:, cols], preferred_element_type=jnp.float32)
                for idx_rows, rows in enumerate(block_rows):
                    total[rows, cols] = part[idx_rows * DOT_ROWS:(idx_rows + 1) * DOT_ROWS]
                return inner

            lax.fori_loop(0, width // DOT_COLS, columns, 0)

        for sign, base, send, recv, g_send, g_recv in streams:
            place = me if sign == 1 else last - me
            chunk = step - place
            rows = pl.ds(pl.multiple_of(base + chunk * SUM_ROWS, SUM_ROWS), SUM_ROWS)
            inside = (chunk >= 0) & (chunk < chunks)
            nxt = me + sign
            prev = me - sign

            @pl.when(inside & (place > 0))
            def _():
                to_peer(total.at[rows], came.at[rows], send.at[chunk], recv.at[chunk], me).wait_recv()

                @pl.when(place < last)
                def _():
                    total[rows, :] = total[rows, :] + came[rows, :]

                @pl.when(place == last)
                def _():
                    update = (total[rows, :] + came[rows, :]).astype(jnp.bfloat16).astype(jnp.float32)
                    out_ref[rows, :] = (hid_ref[rows, :].astype(jnp.float32) + update).astype(jnp.bfloat16)
                    to_peer(out_ref.at[rows], out_ref.at[rows], g_send.at[chunk], g_recv.at[chunk], prev).start()

            @pl.when(inside & (place < last))
            def _():
                to_peer(total.at[rows], came.at[rows], send.at[chunk], recv.at[chunk], nxt).start()

        for sign, base, send, recv, g_send, g_recv in streams:
            place = me if sign == 1 else last - me
            chunk = step - last - (last - place)
            rows = pl.ds(pl.multiple_of(base + chunk * SUM_ROWS, SUM_ROWS), SUM_ROWS)
            prev = me - sign

            @pl.when((chunk >= 0) & (chunk < chunks) & (place < last))
            def _():
                to_peer(out_ref.at[rows], out_ref.at[rows], g_send.at[chunk], g_recv.at[chunk], me).wait_recv()

                @pl.when(place > 0)
                def _():
                    to_peer(out_ref.at[rows], out_ref.at[rows], g_send.at[chunk], g_recv.at[chunk], prev).start()
        return carry

    lax.fori_loop(0, per_dot + chunks + 2 * last, tick, 0)

    def drain(chunk, carry):
        for sign, base, send, recv, g_send, g_recv in streams:
            place = me if sign == 1 else last - me
            rows = pl.ds(pl.multiple_of(base + chunk * SUM_ROWS, SUM_ROWS), SUM_ROWS)

            @pl.when(place < last)
            def _():
                to_peer(total.at[rows], came.at[rows], send.at[chunk], recv.at[chunk], me + sign).wait_send()

            @pl.when(place > 0)
            def _():
                to_peer(out_ref.at[rows], out_ref.at[rows], g_send.at[chunk], g_recv.at[chunk], me - sign).wait_send()
        return carry

    lax.fori_loop(0, chunks, drain, 0)
    sum_small(me, tp_size, part_ref, held, sm_send, sm_recv, small_ref)


def mlp_and_sum(layer, ctx_full, hidden, wo_full, w_gu, w_down, gain, small_part, tp_size):
    rows, width = hidden.shape
    chunks = rows // 2 // SUM_ROWS
    ff_loc = w_down.shape[1]
    vmem = pl.BlockSpec(memory_space=pltpu.VMEM)
    hbm = pl.BlockSpec(memory_space=pl.ANY)
    bf16 = jnp.bfloat16
    return pl.pallas_call(
        lambda *refs: sum_kernel(layer, tp_size, *refs),
        out_shape=(jax.ShapeDtypeStruct(hidden.shape, hidden.dtype), jax.ShapeDtypeStruct(small_part.shape, bf16)),
        in_specs=[hbm] * 5 + [vmem] * 2,
        out_specs=(vmem, vmem),
        scratch_shapes=[
            pltpu.VMEM(ctx_full.shape, bf16),
            pltpu.VMEM((rows, width), bf16),
            pltpu.VMEM((wo_full.shape[1], wo_full.shape[0]) + wo_full.shape[2:], bf16),
            pltpu.VMEM((2, ff_loc, width), bf16),
            pltpu.VMEM((ff_loc, width), bf16),
            pltpu.VMEM((2 * DOT_ROWS, width), bf16),
            pltpu.VMEM((2 * DOT_ROWS, ff_loc), bf16),
            pltpu.VMEM((rows, width), jnp.float32),
            pltpu.VMEM((rows, width), jnp.float32),
            pltpu.VMEM((tp_size,) + small_part.shape, jnp.float32),
            pltpu.SemaphoreType.DMA((4 + tp_size,)),
        ] + [pltpu.SemaphoreType.DMA((chunks,))] * 8 + [pltpu.SemaphoreType.DMA((tp_size - 1,)), pltpu.SemaphoreType.DMA((tp_size,))],
        compiler_params=pltpu.CompilerParams(collective_id=1 + layer, has_side_effects=True, vmem_limit_bytes=SUM_VMEM_BYTES),
        cost_estimate=pl.CostEstimate(flops=160_000_000_000, bytes_accessed=rows * width * 20, transcendentals=0),
        name='mlp_sum',
    )(ctx_full, hidden, wo_full, w_gu, w_down, gain, small_part)


def rms_norm(hidden, gain_vec):
    hid_f32 = hidden.astype(jnp.float32)
    inv_rms = lax.rsqrt(jnp.mean(hid_f32 * hid_f32, axis=-1, keepdims=True) + EPSILON)
    return (hid_f32 * inv_rms * gain_vec).astype(jnp.bfloat16)


def add_residual(hidden, update):
    return (hidden.astype(jnp.float32) + update.astype(jnp.float32)).astype(jnp.bfloat16)


def rope_tables(positions, head_dim):
    half_dim = head_dim // 2
    inv_freq = THETA ** (-jnp.arange(half_dim, dtype=jnp.float32) * 2.0 / head_dim)
    angles = positions.astype(jnp.float32)[:, None] * inv_freq[None, :]
    return jnp.cos(angles), jnp.sin(angles)


def apply_rope(values_in, cos_tab, sin_tab):
    half_dim = values_in.shape[-1] // 2
    lower_half = values_in[..., :half_dim]
    upper_half = values_in[..., half_dim:]
    cos_b = cos_tab[:, None, :]
    sin_b = sin_tab[:, None, :]
    return jnp.concatenate([lower_half * cos_b - upper_half * sin_b, upper_half * cos_b + lower_half * sin_b], axis=-1)


def swiglu(hidden, gain_vec, w_gu):
    normed = rms_norm(hidden, gain_vec)
    gate_up = jnp.einsum('sd,kfd->skf', normed, w_gu, preferred_element_type=jnp.float32)
    gate_val = gate_up[..., 0, :].astype(jnp.bfloat16).astype(jnp.float32)
    up_val = gate_up[..., 1, :].astype(jnp.bfloat16).astype(jnp.float32)
    return (jax.nn.silu(gate_val) * up_val).astype(jnp.bfloat16)


def prompt_attention(queries, keys_in, values_in, allowed):
    attn_scale = queries.shape[-1] ** -0.5
    scores = jnp.einsum('qhe,khe->hqk', queries, keys_in, preferred_element_type=jnp.float32) * attn_scale
    scores = jnp.where(allowed[None], scores, MASKED)
    prob_bf = jax.nn.softmax(scores, axis=-1).astype(jnp.bfloat16)
    return jnp.einsum('hqk,khe->qhe', prob_bf, values_in, preferred_element_type=jnp.float32).astype(jnp.bfloat16)


def decode_attention(queries, k_tok, v_tok, k_layer, v_layer, visible):
    attn_scale = queries.shape[-1] ** -0.5
    cache_scores = jnp.einsum('bhe,bthe->bht', queries, k_layer, preferred_element_type=jnp.float32) * attn_scale
    cache_scores = jnp.where(visible, cache_scores, MASKED)
    self_score = jnp.einsum('bhe,bhe->bh', queries, k_tok, preferred_element_type=jnp.float32) * attn_scale
    row_max = jnp.maximum(jnp.max(cache_scores, axis=-1), self_score)
    cache_exp = jnp.exp(cache_scores - row_max[..., None])
    self_exp = jnp.exp(self_score - row_max)
    denominator = jnp.sum(cache_exp, axis=-1) + self_exp
    cache_prob = (cache_exp / denominator[..., None]).astype(jnp.bfloat16)
    self_prob = (self_exp / denominator).astype(jnp.bfloat16).astype(jnp.float32)
    context = jnp.einsum('bht,bthe->bhe', cache_prob, v_layer, preferred_element_type=jnp.float32) + self_prob[..., None] * v_tok.astype(jnp.float32)
    return context.astype(jnp.bfloat16)


def run_layers(prompt, s_valid, w_qkv_pre, wo_full, w_gu_pre, w_down_pre, gains_pre, tokens, k_cache, v_cache, c_len, w_qkv_dec, w_out_dec, w_gu_dec, w_down_dec, gains_dec, partner_perm, tp_size):
    layers, row_count, cache_len, heads_loc, _, head_dim = k_cache.shape
    width = tokens.shape[1]
    seq_len = prompt.shape[0]
    k_local = k_cache.reshape(layers, row_count, cache_len, heads_loc, head_dim)
    v_local = v_cache.reshape(layers, row_count, cache_len, heads_loc, head_dim)
    wqkv_local = w_qkv_dec.reshape(layers, width, 3, heads_loc, head_dim)
    wout_local = w_out_dec.reshape(layers, heads_loc, head_dim, width)
    cos_dec, sin_dec = rope_tables(c_len, head_dim)
    cache_pos = jnp.arange(cache_len)
    visible = (cache_pos[None, :] < c_len[:, None])[:, None, :]
    write_at = (cache_pos[None, :] == c_len[:, None])[:, :, None, None]
    positions = jnp.arange(seq_len)
    cos_pre, sin_pre = rope_tables(positions, head_dim)
    allowed = (positions[None, :] <= positions[:, None]) & (positions[None, :] < s_valid[:, None])
    wqkv_flat = w_qkv_pre.reshape(layers, width, -1)
    hidden = prompt
    installed, k_next, v_next = [], [], []
    for layer_idx in range(layers):
        normed = rms_norm(hidden, gains_pre[layer_idx, 0])
        qkv_out = jnp.dot(normed, wqkv_flat[layer_idx], preferred_element_type=jnp.float32).reshape(seq_len, 3, heads_loc, head_dim)
        queries = apply_rope(qkv_out[:, 0], cos_pre, sin_pre).astype(jnp.bfloat16)
        keys_new = apply_rope(qkv_out[:, 1], cos_pre, sin_pre).astype(jnp.bfloat16)
        values_new = qkv_out[:, 2].astype(jnp.bfloat16)
        context = prompt_attention(queries, keys_new, values_new, allowed).reshape(seq_len, -1)

        normed_tok = rms_norm(tokens, gains_dec[layer_idx, 0])
        qkv_tok = jnp.einsum('bd,dkhe->bkhe', normed_tok, wqkv_local[layer_idx], preferred_element_type=jnp.float32)
        q_tok = apply_rope(qkv_tok[:, 0], cos_dec, sin_dec).astype(jnp.bfloat16)
        k_tok = apply_rope(qkv_tok[:, 1], cos_dec, sin_dec).astype(jnp.bfloat16)
        v_tok = qkv_tok[:, 2].astype(jnp.bfloat16)
        ctx_tok = decode_attention(q_tok, k_tok, v_tok, k_local[layer_idx], v_local[layer_idx], visible)
        part_tok = jnp.einsum('bhe,hed->bd', ctx_tok, wout_local[layer_idx], preferred_element_type=jnp.float32)
        k_next.append(k_tok)
        v_next.append(v_tok)

        ctx_full, attn_tok = gather_ctx(context, part_tok, tp_size)
        kv_new = jnp.stack([keys_new, values_new])
        if layer_idx > 0:
            kv_new, attn_tok = lax.optimization_barrier((kv_new, attn_tok))
        kv_new = lax.all_to_all(kv_new, 'tp', 2, 2, tiled=True)
        installed.append(lax.ppermute(kv_new, 'side', partner_perm))
        tokens = add_residual(tokens, attn_tok)
        act_tok = swiglu(tokens, gains_dec[layer_idx, 1], w_gu_dec[layer_idx])
        mlp_tok = jnp.einsum('bf,fd->bd', act_tok, w_down_dec[layer_idx], preferred_element_type=jnp.float32)
        hidden, down_tok = mlp_and_sum(layer_idx, ctx_full, hidden, wo_full[layer_idx], w_gu_pre, w_down_pre, gains_pre[layer_idx, 1][None], mlp_tok, tp_size)
        tokens = add_residual(tokens, down_tok)
    hidden, installed[-1] = lax.optimization_barrier((hidden, installed[-1]))
    write_rows = write_at[None]
    k_new = jnp.where(write_rows, jnp.stack(k_next)[:, :, None], k_local).reshape(k_cache.shape)
    v_new = jnp.where(write_rows, jnp.stack(v_next)[:, :, None], v_local).reshape(v_cache.shape)
    return hidden, tokens, installed, k_new, v_new


def gather_wo(w_out, side_size, pair_size):
    layers, heads_loc, head_dim, width = w_out.shape
    rows = heads_loc * head_dim
    copies = side_size * pair_size
    place = lax.axis_index('pair') * side_size + lax.axis_index('side')
    mine = lax.dynamic_index_in_dim(w_out.reshape(layers, copies, rows // copies, width), place, axis=1, keepdims=False)
    line = lax.all_gather(mine.reshape(-1, width), 'tp', axis=0).reshape(-1, layers, rows // copies, width)
    return [lax.all_gather(line[:, layer_idx], ('pair', 'side'), axis=0) for layer_idx in range(layers)]


def solution(mesh):
    tp_size = mesh.shape['tp']
    side_size = mesh.shape['side']
    pair_size = mesh.shape['pair']
    partner_perm = [(src_idx, (src_idx + side_size // 2) % side_size) for src_idx in range(side_size)]
    inst_axes = ('pair', 'side')
    rows_spec = P(inst_axes, None)
    vec_spec = P(inst_axes)
    cache_spec = P(None, inst_axes, None, None, 'tp', None)
    prompt_spec = P(None, inst_axes, None, 'tp', None)
    in_specs = (rows_spec, vec_spec, P(None, None, None, 'tp', None), P(None, 'tp', None, None), P(None, None, 'tp', None), P(None, 'tp', None), P(None, None, None), rows_spec, cache_spec, cache_spec, vec_spec, P(None, None, None, None, 'tp', None), P(None, None, 'tp', None, None), P(None, None, 'tp', None), P(None, 'tp', None), P(None, None, None))
    out_specs = (rows_spec, rows_spec, prompt_spec, prompt_spec, cache_spec, cache_spec)

    def device_fn(prompt_x, s_len, w_qkv_pre, w_out_pre, w_gu_pre, w_down_pre, gain_pre, dec_tokens, k_cache, v_cache, c_len, w_qkv_dec, w_out_dec, w_gu_dec, w_down_dec, gain_dec):
        wo_full = gather_wo(w_out_pre, side_size, pair_size)
        hidden, dec_out, installed, k_cache_new, v_cache_new = run_layers(prompt_x, s_len, w_qkv_pre, wo_full, w_gu_pre, w_down_pre, gain_pre, dec_tokens, k_cache, v_cache, c_len, w_qkv_dec, w_out_dec, w_gu_dec, w_down_dec, gain_dec, partner_perm, tp_size)
        prompt_kv = jnp.stack(installed, axis=1)[:, :, :, :, None, :]
        return hidden, dec_out, prompt_kv[0], prompt_kv[1], k_cache_new, v_cache_new

    return jax.shard_map(device_fn, mesh=mesh, in_specs=in_specs, out_specs=out_specs, check_vma=False)
```

```python
import jax
import jax.numpy as jnp
from jax import lax
from jax.experimental import pallas as pl
from jax.experimental.pallas import tpu as pltpu
from jax.sharding import PartitionSpec as P

EPSILON = 1e-6
THETA = 10000.0
MASKED = -1e30
CTX_ROWS = 128
SUM_ROWS = 32
DOT_ROWS = 128
DOT_COLS = 512
STAGES = 4
FF_COLS = 256
SUM_VMEM_BYTES = 63 * 1024 * 1024
VMEM_BYTES = 56 * 1024 * 1024
MESH = pl.DeviceIdType.MESH


def greet(me, tp_size):
    barrier = pltpu.get_barrier_semaphore()
    for off in range(1, tp_size):
        pl.semaphore_signal(barrier, inc=1, device_id={'tp': lax.rem(me + off, tp_size)}, device_id_type=MESH)
    pl.semaphore_wait(barrier, tp_size - 1)


def to_peer(src, dst, send_sem, recv_sem, peer):
    return pltpu.make_async_remote_copy(src_ref=src, dst_ref=dst, send_sem=send_sem, recv_sem=recv_sem, device_id={'tp': peer}, device_id_type=MESH)


def share_small(me, tp_size, part_ref, held, send_sems, recv_sems):
    for off in range(1, tp_size):
        peer = lax.rem(me + off, tp_size)
        to_peer(part_ref, held.at[me], send_sems.at[off - 1], recv_sems.at[me], peer).start()


def sum_small(me, tp_size, part_ref, held, send_sems, recv_sems, out_ref):
    for off in range(1, tp_size):
        peer = lax.rem(me + off, tp_size)
        copy = to_peer(part_ref, held.at[peer], send_sems.at[off - 1], recv_sems.at[peer], peer)
        copy.wait_send()
        copy.wait_recv()
    held[me] = part_ref[...]
    total = held[0]
    for idx in range(1, tp_size):
        total = total + held[idx]
    out_ref[...] = total.astype(out_ref.dtype)


def ctx_kernel(tp_size, ctx_ref, part_ref, full_ref, small_ref, held, up_send, up_recv, dn_send, dn_recv, sm_send, sm_recv):
    me = lax.axis_index('tp')
    last = tp_size - 1
    chunks = ctx_ref.shape[0] // CTX_ROWS
    greet(me, tp_size)
    share_small(me, tp_size, part_ref, held, sm_send, sm_recv)

    def rows_of(chunk):
        return pl.ds(pl.multiple_of(chunk * CTX_ROWS, CTX_ROWS), CTX_ROWS)

    def tick(step, carry):
        for back in range(tp_size):
            chunk = step - back
            inside = (chunk >= 0) & (chunk < chunks)
            for sign, send, recv in ((1, up_send, up_recv), (-1, dn_send, dn_recv)):
                shard = me - sign * back
                peer = me + sign
                has = inside & (shard >= 0) & (shard <= last)
                more = has & (peer >= 0) & (peer <= last)
                rows = rows_of(chunk)
                if back == 0:
                    @pl.when(more)
                    def _():
                        to_peer(ctx_ref.at[rows], full_ref.at[me, rows], send.at[0, chunk], recv.at[0, chunk], peer).start()
                else:
                    @pl.when(has)
                    def _():
                        to_peer(ctx_ref.at[rows], full_ref.at[shard, rows], send.at[back - 1, chunk], recv.at[back - 1, chunk], me).wait_recv()
                    if back < last:
                        @pl.when(more)
                        def _():
                            to_peer(full_ref.at[shard, rows], full_ref.at[shard, rows], send.at[back, chunk], recv.at[back, chunk], peer).start()
        return carry

    lax.fori_loop(0, chunks + last, tick, 0)
    full_ref[me] = ctx_ref[...]

    def drain(chunk, carry):
        for back in range(last):
            for sign, send, recv in ((1, up_send, up_recv), (-1, dn_send, dn_recv)):
                shard = me - sign * back
                peer = me + sign

                @pl.when((shard >= 0) & (shard <= last) & (peer >= 0) & (peer <= last))
                def _():
                    to_peer(ctx_ref.at[rows_of(chunk)], full_ref.at[me, rows_of(chunk)], send.at[back, chunk], recv.at[back, chunk], peer).wait_send()
        return carry

    lax.fori_loop(0, chunks, drain, 0)
    sum_small(me, tp_size, part_ref, held, sm_send, sm_recv, small_ref)


def gather_ctx(ctx, small_part, tp_size):
    rows, width = ctx.shape
    chunks = rows // CTX_ROWS
    last = tp_size - 1
    vmem = pl.BlockSpec(memory_space=pltpu.VMEM)
    return pl.pallas_call(
        lambda *refs: ctx_kernel(tp_size, *refs),
        out_shape=(jax.ShapeDtypeStruct((tp_size, rows, width), ctx.dtype), jax.ShapeDtypeStruct(small_part.shape, jnp.bfloat16)),
        in_specs=[vmem, vmem],
        out_specs=(vmem, vmem),
        scratch_shapes=[pltpu.VMEM((tp_size,) + small_part.shape, jnp.float32)] + [pltpu.SemaphoreType.DMA((last, chunks))] * 4 + [pltpu.SemaphoreType.DMA((last,)), pltpu.SemaphoreType.DMA((tp_size,))],
        compiler_params=pltpu.CompilerParams(collective_id=0, has_side_effects=True, vmem_limit_bytes=VMEM_BYTES),
        cost_estimate=pl.CostEstimate(flops=70_000_000_000, bytes_accessed=rows * width * 10, transcendentals=0),
        name='ctx_gather',
    )(ctx, small_part)


def sum_kernel(layer, tp_size, ctx_hbm, hid_hbm, wo_hbm, gu_hbm, wd_hbm, gain_ref, part_ref, out_ref, small_ref, ctx_ref, hid_ref, wo_ref, gu_ref, wd_ref, norm_ref, act_ref, total, came, held, in_sems, up_send, up_recv, dn_send, dn_recv, gu_send, gu_recv, gd_send, gd_recv, sm_send, sm_recv):
    me = lax.axis_index('tp')
    last = tp_size - 1
    half = hid_ref.shape[0] // 2
    chunks = half // SUM_ROWS
    per_dot = DOT_ROWS // SUM_ROWS
    width = hid_ref.shape[1]
    ff_loc = wd_ref.shape[0]
    shard = ctx_ref.shape[2]
    loads = [
        pltpu.make_async_copy(ctx_hbm, ctx_ref, in_sems.at[0]),
        pltpu.make_async_copy(hid_hbm, hid_ref, in_sems.at[1]),
        pltpu.make_async_copy(gu_hbm.at[layer], gu_ref, in_sems.at[2]),
        pltpu.make_async_copy(wd_hbm.at[layer], wd_ref, in_sems.at[3]),
    ]
    weight_loads = [pltpu.make_async_copy(wo_hbm.at[:, src], wo_ref.at[src], in_sems.at[4 + src]) for src in range(tp_size)]
    loads = loads[:2] + weight_loads + loads[2:]
    for load in loads:
        load.start()
    greet(me, tp_size)
    share_small(me, tp_size, part_ref, held, sm_send, sm_recv)
    streams = ((1, half, up_send, up_recv, gu_send, gu_recv), (-1, 0, dn_send, dn_recv, gd_send, gd_recv))
    full_ff = ff_loc // FF_COLS
    rest = ff_loc - full_ff * FF_COLS
    first_part = (full_ff + 1) // 2

    def activate(start, size):
        normed = norm_ref[...]
        contract = (((1,), (1,)), ((), ()))
        gate = lax.dot_general(normed, gu_ref[0, pl.ds(start, size), :], contract, preferred_element_type=jnp.float32)
        up = lax.dot_general(normed, gu_ref[1, pl.ds(start, size), :], contract, preferred_element_type=jnp.float32)
        gate = gate.astype(jnp.bfloat16).astype(jnp.float32)
        up = up.astype(jnp.bfloat16).astype(jnp.float32)
        act_ref[:, pl.ds(start, size)] = (jax.nn.silu(gate) * up).astype(jnp.bfloat16)

    def tick(time, carry):
        step = time - per_dot
        pace = per_dot // STAGES
        on_beat = lax.rem(time, pace) == 0
        stage = lax.rem(time, per_dot) // pace
        block = time // per_dot
        working = (time < chunks) & on_beat
        block_rows = [pl.ds(pl.multiple_of(base + block * DOT_ROWS, DOT_ROWS), DOT_ROWS) for base in (half, 0)]

        @pl.when(time == 0)
        def _():
            for load in loads[:-2]:
                load.wait()

        @pl.when(time == pace)
        def _():
            loads[-2].wait()

        @pl.when(time == 3 * pace)
        def _():
            loads[-1].wait()

        @pl.when(working & (stage == 0))
        def _():
            def columns(idx, inner):
                cols = pl.ds(pl.multiple_of(idx * DOT_COLS, DOT_COLS), DOT_COLS)
                attn = None
                for src in range(tp_size):
                    both = jnp.concatenate([ctx_ref[src, rows, :] for rows in block_rows], axis=0)
                    term = jnp.dot(both, wo_ref[src, :, :, cols].reshape(shard, DOT_COLS), preferred_element_type=jnp.float32)
                    attn = term if attn is None else attn + term
                attn = attn.astype(jnp.bfloat16).astype(jnp.float32)
                for idx_rows, rows in enumerate(block_rows):
                    old = hid_ref[rows, cols].astype(jnp.float32)
                    hid_ref[rows, cols] = (old + attn[idx_rows * DOT_ROWS:(idx_rows + 1) * DOT_ROWS]).astype(jnp.bfloat16)
                return inner

            lax.fori_loop(0, width // DOT_COLS, columns, 0)
            for idx_rows, rows in enumerate(block_rows):
                for sub in range(0, DOT_ROWS, 32):
                    piece = pl.ds(pl.multiple_of(rows.start + sub, 32), 32)
                    hid = hid_ref[piece, :].astype(jnp.float32)
                    inv_rms = lax.rsqrt(jnp.mean(hid * hid, axis=-1, keepdims=True) + EPSILON)
                    norm_ref[idx_rows * DOT_ROWS + sub:idx_rows * DOT_ROWS + sub + 32, :] = (hid * inv_rms * gain_ref[...]).astype(jnp.bfloat16)

        @pl.when(working & ((stage == 1) | (stage == 2)))
        def _():
            low = (stage - 1) * first_part
            high = first_part + (stage - 1) * (full_ff - first_part)

            def features(idx, inner):
                activate(pl.multiple_of(idx * FF_COLS, FF_COLS), FF_COLS)
                return inner

            lax.fori_loop(low, high, features, 0)

        if rest:
            @pl.when(working & (stage == 2))
            def _():
                activate(full_ff * FF_COLS, rest)

        @pl.when(working & (stage == 3))
        def _():
            def columns(idx, inner):
                cols = pl.ds(pl.multiple_of(idx * DOT_COLS, DOT_COLS), DOT_COLS)
                part = jnp.dot(act_ref[...], wd_ref[:, cols], preferred_element_type=jnp.float32)
                for idx_rows, rows in enumerate(block_rows):
                    total[rows, cols] = part[idx_rows * DOT_ROWS:(idx_rows + 1) * DOT_ROWS]
                return inner

            lax.fori_loop(0, width // DOT_COLS, columns, 0)

        for sign, base, send, recv, g_send, g_recv in streams:
            place = me if sign == 1 else last - me
            chunk = step - place
            rows = pl.ds(pl.multiple_of(base + chunk * SUM_ROWS, SUM_ROWS), SUM_ROWS)
            inside = (chunk >= 0) & (chunk < chunks)
            nxt = me + sign
            prev = me - sign

            @pl.when(inside & (place > 0))
            def _():
                to_peer(total.at[rows], came.at[rows], send.at[chunk], recv.at[chunk], me).wait_recv()

                @pl.when(place < last)
                def _():
                    total[rows, :] = total[rows, :] + came[rows, :]

                @pl.when(place == last)
                def _():
                    update = (total[rows, :] + came[rows, :]).astype(jnp.bfloat16).astype(jnp.float32)
                    out_ref[rows, :] = (hid_ref[rows, :].astype(jnp.float32) + update).astype(jnp.bfloat16)
                    to_peer(out_ref.at[rows], out_ref.at[rows], g_send.at[chunk], g_recv.at[chunk], prev).start()

            @pl.when(inside & (place < last))
            def _():
                to_peer(total.at[rows], came.at[rows], send.at[chunk], recv.at[chunk], nxt).start()

        for sign, base, send, recv, g_send, g_recv in streams:
            place = me if sign == 1 else last - me
            chunk = step - last - (last - place)
            rows = pl.ds(pl.multiple_of(base + chunk * SUM_ROWS, SUM_ROWS), SUM_ROWS)
            prev = me - sign

            @pl.when((chunk >= 0) & (chunk < chunks) & (place < last))
            def _():
                to_peer(out_ref.at[rows], out_ref.at[rows], g_send.at[chunk], g_recv.at[chunk], me).wait_recv()

                @pl.when(place > 0)
                def _():
                    to_peer(out_ref.at[rows], out_ref.at[rows], g_send.at[chunk], g_recv.at[chunk], prev).start()
        return carry

    lax.fori_loop(0, per_dot + chunks + 2 * last, tick, 0)

    def drain(chunk, carry):
        for sign, base, send, recv, g_send, g_recv in streams:
            place = me if sign == 1 else last - me
            rows = pl.ds(pl.multiple_of(base + chunk * SUM_ROWS, SUM_ROWS), SUM_ROWS)

            @pl.when(place < last)
            def _():
                to_peer(total.at[rows], came.at[rows], send.at[chunk], recv.at[chunk], me + sign).wait_send()

            @pl.when(place > 0)
            def _():
                to_peer(out_ref.at[rows], out_ref.at[rows], g_send.at[chunk], g_recv.at[chunk], me - sign).wait_send()
        return carry

    lax.fori_loop(0, chunks, drain, 0)
    sum_small(me, tp_size, part_ref, held, sm_send, sm_recv, small_ref)


def mlp_and_sum(layer, ctx_full, hidden, wo_full, w_gu, w_down, gain, small_part, tp_size):
    rows, width = hidden.shape
    chunks = rows // 2 // SUM_ROWS
    ff_loc = w_down.shape[1]
    vmem = pl.BlockSpec(memory_space=pltpu.VMEM)
    hbm = pl.BlockSpec(memory_space=pl.ANY)
    bf16 = jnp.bfloat16
    return pl.pallas_call(
        lambda *refs: sum_kernel(layer, tp_size, *refs),
        out_shape=(jax.ShapeDtypeStruct(hidden.shape, hidden.dtype), jax.ShapeDtypeStruct(small_part.shape, bf16)),
        in_specs=[hbm] * 5 + [vmem] * 2,
        out_specs=(vmem, vmem),
        scratch_shapes=[
            pltpu.VMEM(ctx_full.shape, bf16),
            pltpu.VMEM((rows, width), bf16),
            pltpu.VMEM((wo_full.shape[1], wo_full.shape[0]) + wo_full.shape[2:], bf16),
            pltpu.VMEM((2, ff_loc, width), bf16),
            pltpu.VMEM((ff_loc, width), bf16),
            pltpu.VMEM((2 * DOT_ROWS, width), bf16),
            pltpu.VMEM((2 * DOT_ROWS, ff_loc), bf16),
            pltpu.VMEM((rows, width), jnp.float32),
            pltpu.VMEM((rows, width), jnp.float32),
            pltpu.VMEM((tp_size,) + small_part.shape, jnp.float32),
            pltpu.SemaphoreType.DMA((4 + tp_size,)),
        ] + [pltpu.SemaphoreType.DMA((chunks,))] * 8 + [pltpu.SemaphoreType.DMA((tp_size - 1,)), pltpu.SemaphoreType.DMA((tp_size,))],
        compiler_params=pltpu.CompilerParams(collective_id=1 + layer, has_side_effects=True, vmem_limit_bytes=SUM_VMEM_BYTES),
        cost_estimate=pl.CostEstimate(flops=160_000_000_000, bytes_accessed=rows * width * 20, transcendentals=0),
        name='mlp_sum',
    )(ctx_full, hidden, wo_full, w_gu, w_down, gain, small_part)


def rms_norm(hidden, gain_vec):
    hid_f32 = hidden.astype(jnp.float32)
    inv_rms = lax.rsqrt(jnp.mean(hid_f32 * hid_f32, axis=-1, keepdims=True) + EPSILON)
    return (hid_f32 * inv_rms * gain_vec).astype(jnp.bfloat16)


def add_residual(hidden, update):
    return (hidden.astype(jnp.float32) + update.astype(jnp.float32)).astype(jnp.bfloat16)


def rope_tables(positions, head_dim):
    half_dim = head_dim // 2
    inv_freq = THETA ** (-jnp.arange(half_dim, dtype=jnp.float32) * 2.0 / head_dim)
    angles = positions.astype(jnp.float32)[:, None] * inv_freq[None, :]
    return jnp.cos(angles), jnp.sin(angles)


def apply_rope(values_in, cos_tab, sin_tab):
    half_dim = values_in.shape[-1] // 2
    lower_half = values_in[..., :half_dim]
    upper_half = values_in[..., half_dim:]
    cos_b = cos_tab[:, None, :]
    sin_b = sin_tab[:, None, :]
    return jnp.concatenate([lower_half * cos_b - upper_half * sin_b, upper_half * cos_b + lower_half * sin_b], axis=-1)


def swiglu(hidden, gain_vec, w_gu):
    normed = rms_norm(hidden, gain_vec)
    gate_up = jnp.einsum('sd,kfd->skf', normed, w_gu, preferred_element_type=jnp.float32)
    gate_val = gate_up[..., 0, :].astype(jnp.bfloat16).astype(jnp.float32)
    up_val = gate_up[..., 1, :].astype(jnp.bfloat16).astype(jnp.float32)
    return (jax.nn.silu(gate_val) * up_val).astype(jnp.bfloat16)


def prompt_attention(queries, keys_in, values_in, allowed):
    attn_scale = queries.shape[-1] ** -0.5
    scores = jnp.einsum('qhe,khe->hqk', queries, keys_in, preferred_element_type=jnp.float32) * attn_scale
    scores = jnp.where(allowed[None], scores, MASKED)
    prob_bf = jax.nn.softmax(scores, axis=-1).astype(jnp.bfloat16)
    return jnp.einsum('hqk,khe->qhe', prob_bf, values_in, preferred_element_type=jnp.float32).astype(jnp.bfloat16)


def decode_attention(queries, k_tok, v_tok, k_layer, v_layer, visible):
    attn_scale = queries.shape[-1] ** -0.5
    cache_scores = jnp.einsum('bhe,bthe->bht', queries, k_layer, preferred_element_type=jnp.float32) * attn_scale
    cache_scores = jnp.where(visible, cache_scores, MASKED)
    self_score = jnp.einsum('bhe,bhe->bh', queries, k_tok, preferred_element_type=jnp.float32) * attn_scale
    row_max = jnp.maximum(jnp.max(cache_scores, axis=-1), self_score)
    cache_exp = jnp.exp(cache_scores - row_max[..., None])
    self_exp = jnp.exp(self_score - row_max)
    denominator = jnp.sum(cache_exp, axis=-1) + self_exp
    cache_prob = (cache_exp / denominator[..., None]).astype(jnp.bfloat16)
    self_prob = (self_exp / denominator).astype(jnp.bfloat16).astype(jnp.float32)
    context = jnp.einsum('bht,bthe->bhe', cache_prob, v_layer, preferred_element_type=jnp.float32) + self_prob[..., None] * v_tok.astype(jnp.float32)
    return context.astype(jnp.bfloat16)


def run_layers(prompt, s_valid, w_qkv_pre, wo_full, w_gu_pre, w_down_pre, gains_pre, tokens, k_cache, v_cache, c_len, w_qkv_dec, w_out_dec, w_gu_dec, w_down_dec, gains_dec, partner_perm, tp_size):
    layers, row_count, cache_len, heads_loc, _, head_dim = k_cache.shape
    width = tokens.shape[1]
    seq_len = prompt.shape[0]
    k_local = k_cache.reshape(layers, row_count, cache_len, heads_loc, head_dim)
    v_local = v_cache.reshape(layers, row_count, cache_len, heads_loc, head_dim)
    wqkv_local = w_qkv_dec.reshape(layers, width, 3, heads_loc, head_dim)
    wout_local = w_out_dec.reshape(layers, heads_loc, head_dim, width)
    cos_dec, sin_dec = rope_tables(c_len, head_dim)
    cache_pos = jnp.arange(cache_len)
    visible = (cache_pos[None, :] < c_len[:, None])[:, None, :]
    write_at = (cache_pos[None, :] == c_len[:, None])[:, :, None, None]
    positions = jnp.arange(seq_len)
    cos_pre, sin_pre = rope_tables(positions, head_dim)
    allowed = (positions[None, :] <= positions[:, None]) & (positions[None, :] < s_valid[:, None])
    wqkv_flat = w_qkv_pre.reshape(layers, width, -1)
    hidden = prompt
    installed, k_next, v_next = [], [], []
    for layer_idx in range(layers):
        normed = rms_norm(hidden, gains_pre[layer_idx, 0])
        qkv_out = jnp.dot(normed, wqkv_flat[layer_idx], preferred_element_type=jnp.float32).reshape(seq_len, 3, heads_loc, head_dim)
        queries = apply_rope(qkv_out[:, 0], cos_pre, sin_pre).astype(jnp.bfloat16)
        keys_new = apply_rope(qkv_out[:, 1], cos_pre, sin_pre).astype(jnp.bfloat16)
        values_new = qkv_out[:, 2].astype(jnp.bfloat16)
        context = prompt_attention(queries, keys_new, values_new, allowed).reshape(seq_len, -1)

        normed_tok = rms_norm(tokens, gains_dec[layer_idx, 0])
        qkv_tok = jnp.einsum('bd,dkhe->bkhe', normed_tok, wqkv_local[layer_idx], preferred_element_type=jnp.float32)
        q_tok = apply_rope(qkv_tok[:, 0], cos_dec, sin_dec).astype(jnp.bfloat16)
        k_tok = apply_rope(qkv_tok[:, 1], cos_dec, sin_dec).astype(jnp.bfloat16)
        v_tok = qkv_tok[:, 2].astype(jnp.bfloat16)
        ctx_tok = decode_attention(q_tok, k_tok, v_tok, k_local[layer_idx], v_local[layer_idx], visible)
        part_tok = jnp.einsum('bhe,hed->bd', ctx_tok, wout_local[layer_idx], preferred_element_type=jnp.float32)
        k_next.append(k_tok)
        v_next.append(v_tok)

        ctx_full, attn_tok = gather_ctx(context, part_tok, tp_size)
        kv_new = jnp.stack([keys_new, values_new])
        if layer_idx == 0:
            kv_new = lax.all_to_all(kv_new, 'tp', 2, 2, tiled=True)
            installed.append(lax.ppermute(kv_new, 'side', partner_perm))
        else:
            kv_new = lax.ppermute(kv_new, 'side', partner_perm)
            kv_new, attn_tok = lax.optimization_barrier((kv_new, attn_tok))
            installed.append(lax.all_to_all(kv_new, 'tp', 2, 2, tiled=True))
        tokens = add_residual(tokens, attn_tok)
        act_tok = swiglu(tokens, gains_dec[layer_idx, 1], w_gu_dec[layer_idx])
        mlp_tok = jnp.einsum('bf,fd->bd', act_tok, w_down_dec[layer_idx], preferred_element_type=jnp.float32)
        hidden, down_tok = mlp_and_sum(layer_idx, ctx_full, hidden, wo_full[layer_idx], w_gu_pre, w_down_pre, gains_pre[layer_idx, 1][None], mlp_tok, tp_size)
        tokens = add_residual(tokens, down_tok)
    hidden, installed[-1] = lax.optimization_barrier((hidden, installed[-1]))
    write_rows = write_at[None]
    k_new = jnp.where(write_rows, jnp.stack(k_next)[:, :, None], k_local).reshape(k_cache.shape)
    v_new = jnp.where(write_rows, jnp.stack(v_next)[:, :, None], v_local).reshape(v_cache.shape)
    return hidden, tokens, installed, k_new, v_new


def gather_wo(w_out, side_size, pair_size):
    layers, heads_loc, head_dim, width = w_out.shape
    rows = heads_loc * head_dim
    copies = side_size * pair_size
    place = lax.axis_index('pair') * side_size + lax.axis_index('side')
    mine = lax.dynamic_index_in_dim(w_out.reshape(layers, copies, rows // copies, width), place, axis=1, keepdims=False)
    line = lax.all_gather(mine.reshape(-1, width), 'tp', axis=0).reshape(-1, layers, rows // copies, width)
    return [lax.all_gather(line[:, layer_idx], ('pair', 'side'), axis=0) for layer_idx in range(layers)]


def solution(mesh):
    tp_size = mesh.shape['tp']
    side_size = mesh.shape['side']
    pair_size = mesh.shape['pair']
    partner_perm = [(src_idx, (src_idx + side_size // 2) % side_size) for src_idx in range(side_size)]
    inst_axes = ('pair', 'side')
    rows_spec = P(inst_axes, None)
    vec_spec = P(inst_axes)
    cache_spec = P(None, inst_axes, None, None, 'tp', None)
    prompt_spec = P(None, inst_axes, None, 'tp', None)
    in_specs = (rows_spec, vec_spec, P(None, None, None, 'tp', None), P(None, 'tp', None, None), P(None, None, 'tp', None), P(None, 'tp', None), P(None, None, None), rows_spec, cache_spec, cache_spec, vec_spec, P(None, None, None, None, 'tp', None), P(None, None, 'tp', None, None), P(None, None, 'tp', None), P(None, 'tp', None), P(None, None, None))
    out_specs = (rows_spec, rows_spec, prompt_spec, prompt_spec, cache_spec, cache_spec)

    def device_fn(prompt_x, s_len, w_qkv_pre, w_out_pre, w_gu_pre, w_down_pre, gain_pre, dec_tokens, k_cache, v_cache, c_len, w_qkv_dec, w_out_dec, w_gu_dec, w_down_dec, gain_dec):
        wo_full = gather_wo(w_out_pre, side_size, pair_size)
        hidden, dec_out, installed, k_cache_new, v_cache_new = run_layers(prompt_x, s_len, w_qkv_pre, wo_full, w_gu_pre, w_down_pre, gain_pre, dec_tokens, k_cache, v_cache, c_len, w_qkv_dec, w_out_dec, w_gu_dec, w_down_dec, gain_dec, partner_perm, tp_size)
        prompt_kv = jnp.stack(installed, axis=1)[:, :, :, :, None, :]
        return hidden, dec_out, prompt_kv[0], prompt_kv[1], k_cache_new, v_cache_new

    return jax.shard_map(device_fn, mesh=mesh, in_specs=in_specs, out_specs=out_specs, check_vma=False)
```
